32 devices in a mesh: grp: 4 (over y, x), mem: 8 (over z, core).
Axes of the slice: x: 2, y: 2, z: 4, core: 2. Of those that a mesh axis runs over, the one named last changes fastest.
Arguments:
- params: float32 [4, 2048, 2048], P('grp', 'mem'), may hold values from -6 to 6
- estimate: float32 [4, 2048, 2048], P('grp', 'mem'), may hold values from -6 to 6
- mixed_sum: float32 [4, 2048, 2048], P('grp', 'mem'), may hold values from -6 to 6
- activations: bfloat16 [32768, 2048], P(('grp', 'mem')), may hold values from -6 to 6
- out_grads: bfloat16 [32768, 2048], P(('grp', 'mem')), may hold values from -6 to 6
- exponents: int32 [4, 32], P('grp', 'mem'), may hold values from 0 to 3
- edge_weight: float32 [4], replicated, may hold values from 0.1 to 0.45
Outputs:
- new_params: float32 [4, 2048, 2048], P('grp', 'mem')
- new_estimate: float32 [4, 2048, 2048], P('grp', 'mem')
- new_mixed: float32 [4, 2048, 2048], P('grp', 'mem')
The draws below stay inside these ranges and needn't reach their ends.
All inputs are finite; a program needn't handle non-finite values.
Results may differ from the reference program's by a relative error of at most 0.01.
Values may be sent and summed in bfloat16 or wider, within the bound.
A program may use at most 128 MiB of HBM per device.

```python
import math
import jax
import jax.numpy as jnp
from jax import lax

D = 2048
INNER = 2048
TOK_DEV = 1024
BLOCK = 64
GROUPS = 4
ROWS = 32768
N_MEM = 8


def plant(entries, key, low, top_value):
    spot = [jax.random.randint(jax.random.fold_in(key, axis), (), 0, length) for axis, length in enumerate(entries.shape)]
    longest = entries.shape.index(max(entries.shape))
    neighbour = spot[:longest] + [(spot[longest] + 1) % entries.shape[longest]] + spot[longest + 1:]
    return entries.at[tuple(spot)].set(low).at[tuple(neighbour)].set(top_value)


def strengthened(array, stream_key, source, target, blocks, factor):
    def block_of(dim):
        return (jnp.arange(array.shape[dim]) // (array.shape[dim] // blocks)).reshape((-1,) + (1,) * (array.ndim - 1 - dim))

    first = jax.random.permutation(stream_key, blocks)[block_of(target)]
    second = (block_of(target) + blocks // 2) % blocks
    return jnp.where((block_of(source) == first) | (block_of(source) == second), factor * array, array)


def block_scale(stream_key, shape, cuts, smallest, largest):
    loudness, own = 1.0, jax.random.fold_in(stream_key, 6)
    for dim, shards_of in cuts:
        steps = jnp.exp(jax.random.uniform(jax.random.fold_in(own, dim), (shards_of,), jnp.float32, smallest / len(cuts), largest / len(cuts)))
        loudness = loudness * jnp.repeat(steps, shape[dim] // shards_of).reshape([-1 if axis == dim else 1 for axis in range(len(shape))])
    return loudness


def scatter_about(key, extent, scale, bound, pieces=(), dtype=jnp.bfloat16):
    drawn = jax.random.normal(key, extent, jnp.float32) * scale
    if len(pieces) > 0:
        drawn = block_scale(key, extent, pieces, -0.22, 0.18) * drawn
    return jnp.clip(drawn, min=-bound, max=bound).astype(dtype)


def gaussian_with(own_key, extent, spread, most, pieces, heavy, dtype=jnp.bfloat16):
    entries = spread * jax.random.normal(own_key, extent, jnp.float32)
    if pieces:
        entries = entries * block_scale(own_key, extent, pieces, -0.22, 0.18)
    return jnp.clip(strengthened(entries, jax.random.fold_in(own_key, 3), *heavy), -most, most).astype(dtype)


def setup_inputs(seed: int = 0) -> dict:
    key_list = jax.random.split(jax.random.key(seed), 8)
    params = scatter_about(key_list[0], (GROUPS, D, INNER), 1.0, 6.0, ((0, 4), (1, 8)), jnp.float32)
    estimate = scatter_about(key_list[1], (GROUPS, D, INNER), 1.0, 6.0, ((0, 4), (1, 8)), jnp.float32)
    mixed_sum = scatter_about(key_list[2], (GROUPS, D, INNER), 1.0, 6.0, ((0, 4), (1, 8)), jnp.float32)
    activations = gaussian_with(key_list[3], (ROWS, D), 1.0, 6.0, ((0, 32),), (0, 1, 32, 2.75))
    out_grads = scatter_about(key_list[4], (ROWS, INNER), 1.0, 6.0, ((0, 32),))
    exponents = plant(jax.random.randint(key_list[5], (GROUPS, D // BLOCK), 0, 4), jax.random.fold_in(key_list[5], 1), 0, 3).astype(jnp.int32)
    edge_weight = jnp.clip(jax.random.uniform(key_list[6], (GROUPS,), jnp.float32, 0.1, 0.45), 0.1, 0.45)
    return dict(params=params, estimate=estimate, mixed_sum=mixed_sum, activations=activations, out_grads=out_grads, exponents=exponents, edge_weight=edge_weight)


step_size = 0.5
mixing_rate = 0.4

def reference(params, estimate, mixed_sum, activations, out_grads, exponents, edge_weight):
    groups = params.shape[0]
    group_acts = activations.reshape(groups, N_MEM, TOK_DEV, D)
    group_outs = out_grads.reshape(groups, N_MEM, TOK_DEV, INNER)

    def group_gradient(blocks):

        def accumulate(running, member):
            partial_value = lax.dot_general(member[0], member[1], (((0,), (0,)), ((), ())), preferred_element_type=jnp.float32)
            rounded = lax.optimization_barrier(partial_value.astype(jnp.bfloat16))
            return (running + rounded.astype(jnp.float32), None)
        running, _ = lax.scan(accumulate, jnp.zeros((D, INNER), jnp.float32), blocks)
        return running
    gradient = lax.map(group_gradient, (group_acts, group_outs))
    factor = step_size / math.sqrt(N_MEM * TOK_DEV)
    stepped = params - factor * gradient
    change = stepped - estimate
    scales = jnp.exp2(exponents.astype(jnp.float32))[:, :, None, None]
    blocked = change.reshape(groups, D // BLOCK, BLOCK, INNER)
    levels = lax.optimization_barrier(jnp.clip(blocked / scales, -1.0, 1.0).astype(jnp.bfloat16))
    compressed = (levels.astype(jnp.float32) * scales).astype(jnp.bfloat16).reshape(groups, D, INNER)
    own_piece = compressed.astype(jnp.float32)
    new_estimate = estimate + own_piece
    left_piece = jnp.roll(compressed, 1, axis=0).astype(jnp.float32)
    right_piece = jnp.roll(compressed, -1, axis=0).astype(jnp.float32)
    weight_right = edge_weight
    weight_left = jnp.roll(edge_weight, 1)
    weight_self = 1.0 - weight_left - weight_right
    new_mixed = mixed_sum + weight_self[:, None, None] * own_piece
    new_mixed = new_mixed + weight_left[:, None, None] * left_piece
    new_mixed = new_mixed + weight_right[:, None, None] * right_piece
    new_params = stepped + mixing_rate * (new_mixed - new_estimate)
    return (new_params, new_estimate, new_mixed)
```

```python
import functools
import math

import jax
import jax.numpy as jnp
from jax import lax
from jax.experimental import pallas as pl
from jax.experimental.pallas import tpu as pltpu
from jax.sharding import PartitionSpec as P

step_size = 0.5
mixing_rate = 0.4
CHUNKS = 16
DEPTH = 3
LAG = 2
RELAY = 2
GOSSIP = 4
DIRECT = 1
PIECES = 4
SPLIT = 2
SLOTS = 4
RING = 8
MESH = pl.DeviceIdType.MESH
f32 = jnp.float32
bf16 = jnp.bfloat16


def kernel(
    cfg,
    params, estimate, mixed, acts, grads, exponents, edges,
    out_params, out_estimate, out_mixed,
    act_v, act_t, grad_v, par_v, est_v, mix_v,
    mine, give, got, line_out, line_in, own, near, far,
    act_sem, grad_sem, load_sem,
    pair_s, half_r, pair_r, line_s, line_r, near_s, near_r, far_s, far_r,
):
    members, groups, chunks, rows, width, tokens, factor = cfg
    chips = members // 2
    pairs = chips // 2
    steps = chips - 1
    cols = width // chunks
    g = lax.axis_index("grp")
    m = lax.axis_index("mem")
    chip, core = m // 2, m % 2
    other = 1 - core
    sibling = chip * 2 + other
    line_to = [
        lax.rem(chip + 1, chips) * 2 + core,
        lax.rem(chip + chips - 1, chips) * 2 + core,
    ]
    place = [chip, chips - 1 - chip]
    odd = g % 2
    near_to = lax.rem(g + groups + 1 - 2 * odd, groups)
    far_to = lax.rem(g + groups - 1 + 2 * odd, groups)
    onward = lax.rem(g + groups + 2 - 4 * odd, groups)
    backward = lax.rem(g + groups - 2 + 4 * odd, groups)

    begin = [2 * s + 3 if s else 0 for s in range(pairs)]
    for s in range(pairs, steps):
        begin.append(begin[-1] + 1)
    first = jnp.int32(0)
    last = 0
    for c in range(chips):
        after = max(begin[steps - p] + LAG * p for p in (c, chips - 1 - c) if p > 0)
        after += after % 2
        first = jnp.where(chip == c, after, first)
        last = max(last, after)

    def load_block(block, sem):
        return pltpu.make_async_copy(
            acts.at[:, pl.ds(pl.multiple_of(block * rows, rows), rows)], act_v.at[block], act_sem.at[sem]
        )

    def lanes(j):
        return pl.ds(pl.multiple_of(j * cols, cols), cols)

    bounds = [0, 2]
    while bounds[-1] < chunks:
        bounds.append(min(2 * bounds[-1], chunks))

    def grad_copy(k):
        at = pl.ds(bounds[k] * cols, (bounds[k + 1] - bounds[k]) * cols)
        return pltpu.make_async_copy(grads.at[:, at], grad_v.at[:, at], grad_sem.at[k])

    loads = [
        pltpu.make_async_copy(src.at[0], dst, load_sem.at[k])
        for k, (src, dst) in enumerate(((params, par_v), (estimate, est_v), (mixed, mix_v)))
    ]

    def to_sibling(at, recv_sem):
        return pltpu.make_async_remote_copy(
            src_ref=give.at[at] if at else give, dst_ref=got.at[at] if at else got,
            send_sem=pair_s, recv_sem=recv_sem,
            device_id={"mem": sibling}, device_id_type=MESH,
        )

    def half_copy(j, which):
        return to_sibling((j, which), half_r.at[j, which])

    def pair_copy(b, j):
        return to_sibling((b * (chunks // 2) + j,), pair_r.at[b, j % SLOTS])

    ring = line_r.shape[2]

    def line_copy(way, s, j):
        return pltpu.make_async_remote_copy(
            src_ref=line_out.at[way, s * chunks + j], dst_ref=line_in.at[way, s * chunks + j],
            send_sem=line_s.at[way, s, j % DEPTH], recv_sem=line_r.at[way, s, j % ring],
            device_id={"mem": line_to[way]}, device_id_type=MESH,
        )

    def to_group(src, dst, peer, send_sem, recv_sem, at):
        return pltpu.make_async_remote_copy(
            src_ref=src.at[at] if at else src, dst_ref=dst.at[at] if at else dst,
            send_sem=send_sem, recv_sem=recv_sem,
            device_id={"grp": peer}, device_id_type=MESH,
        )

    span = near_r.shape[0]
    relayed = chunks - DIRECT

    def near_copy(j):
        return to_group(own, near, near_to, near_s, near_r.at[j % span], (j,))

    def relay_copy(j):
        return to_group(near, far, onward, far_s, far_r.at[j % span], (j,))

    def far_copy(j):
        return to_group(own, far, far_to, far_s, far_r.at[span + j - relayed], (j,))

    def guarded(run, j, count, least=0):
        @pl.when(jnp.logical_and(j >= least, j < count))
        def _():
            run(j)

    lead_which = jnp.where(chip < pairs, 1, 0)
    lead = jnp.where(chip < pairs, chips - 1, 0)
    trail = chips - 1 - lead

    grad_copy(0).start()
    load_block(lead * 2 + other, 0).start()
    load_block(lead * 2 + core, 1).start()

    barrier = pltpu.get_barrier_semaphore()
    for peer in ({"mem": sibling}, {"grp": near_to}, {"grp": far_to}, {"grp": onward}, {"grp": backward}):
        pl.semaphore_signal(barrier, inc=1, device_id=peer, device_id_type=MESH)
    for way in (0, 1):
        @pl.when(place[way] < chips - 1)
        def _(way=way):
            pl.semaphore_signal(
                barrier, inc=1, device_id={"mem": line_to[way]}, device_id_type=MESH
            )
    greeted = 7 - jnp.where(chip == 0, 1, 0) - jnp.where(chip == chips - 1, 1, 0)

    load_block(trail * 2 + other, 2).start()
    load_block(trail * 2 + core, 3).start()
    grad_copy(1).start()

    def turn(block):
        act_t[block] = act_v[block].T

    def product(dest, parity, j):
        return jnp.dot(
            act_t[dest * 2 + parity],
            grad_v[:, pl.ds(pl.multiple_of(2 * j * cols, 2 * cols), 2 * cols)],
            preferred_element_type=f32,
        ).astype(bf16)

    def give_half(dest, which, j):
        give[j, which] = product(dest, other, j)
        half_copy(j, which).start()

    def keep_half(dest, which, j):
        mine[j, which] = product(dest, core, j)

    def multiply(b, j):
        i = b * (chunks // 2) + j
        if b == 0:
            for k in range(len(bounds) - 1):
                @pl.when(2 * j == bounds[k])
                def _(k=k):
                    grad_copy(k).wait()
        for which, dest in ((0, b), (1, chips - 1 - b)):
            give[i, which] = product(dest, other, j)
        pair_copy(b, j).start()
        for which, dest in ((0, b), (1, chips - 1 - b)):
            mine[i, which] = product(dest, core, j)

    def exchanged(b, j):
        pair_copy(b, j).wait_recv()

    def half_of(half):
        return pl.ds(half * cols, cols)

    def pair_sum(i, which, half):
        return mine[i, which, :, half_of(half)].astype(f32) + got[i, which, :, half_of(half)].astype(f32)

    def pass_on(way, s, j, half, least=0):
        far_dest = steps - s
        b = min(s, steps - s)
        which = (1 if far_dest >= pairs else 0) ^ way
        i = b * (chunks // 2) + j // 2
        slot = s * chunks + j

        @pl.when(jnp.logical_and(far_dest > place[way], jnp.logical_and(j >= least, j < chunks)))
        def _():
            @pl.when(j >= DEPTH)
            def _():
                line_copy(way, s, j - DEPTH).wait_send()

            @pl.when(place[way] == 0)
            def _():
                line_out[way, slot] = pair_sum(i, which, half).astype(bf16)

            @pl.when(place[way] > 0)
            def _():
                line_copy(way, s, j).wait_recv()
                line_out[way, slot] = (
                    pair_sum(i, which, half) + line_in[way, slot].astype(f32)
                ).astype(bf16)

            line_copy(way, s, j).start()

    weight_right = edges[g]
    weight_left = edges[lax.rem(g + groups - 1, groups)]
    weight_self = 1.0 - weight_left - weight_right
    weight_near = jnp.where(odd == 1, weight_left, weight_right)
    weight_far = jnp.where(odd == 1, weight_right, weight_left)
    blocks = exponents.shape[1]
    block_rows = rows // blocks
    own_which = jnp.where(chip >= pairs, 1, 0)
    own_block = jnp.where(chip >= pairs, chips - 1 - chip, chip)

    def compress(half, j):
        slot_of = [(steps - place[way]) * chunks + j for way in (0, 1)]
        @pl.when(j == 0)
        def _():
            for copy in loads:
                copy.wait()

        for way in (0, 1):
            @pl.when(place[way] == 0)
            def _(way=way):
                line_in[way, slot_of[way]] = jnp.zeros((rows, cols), bf16)

            @pl.when(place[way] > 0)
            def _(way=way):
                line_copy(way, steps - place[way], j).wait_recv()
        i = own_block * (chunks // 2) + j // 2
        for b in range(blocks):
            exponent = exponents[0, b]
            scale = (jnp.int32(1) << exponent).astype(f32)
            inverse = (jnp.int32(1) << (15 - exponent)).astype(f32) * (2.0 ** -15)
            at = pl.ds(b * block_rows, block_rows)
            gradient = (
                mine[i, own_which, at, half_of(half)].astype(f32)
                + got[i, own_which, at, half_of(half)].astype(f32)
                + line_in[0, slot_of[0], at, :].astype(f32)
                + line_in[1, slot_of[1], at, :].astype(f32)
            )
            stepped = par_v[at, lanes(j)] - factor * gradient
            levels = jnp.clip((stepped - est_v[at, lanes(j)]) * inverse, -1.0, 1.0).astype(bf16)
            own[j, at, :] = (levels.astype(f32) * scale).astype(bf16)
            out_params[0, at, lanes(j)] = stepped
        @pl.when(j >= relayed)
        def _():
            far_copy(j).start()

        near_copy(j).start()
        compressed = own[j].astype(f32)
        out_estimate[0, :, lanes(j)] = est_v[:, lanes(j)] + compressed
        out_mixed[0, :, lanes(j)] = mix_v[:, lanes(j)] + weight_self * compressed

    def forward(j):
        near_copy(j).wait_recv()

        @pl.when(j < relayed)
        def _():
            relay_copy(j).start()

    def finish(j):
        @pl.when(j < relayed)
        def _():
            relay_copy(j).wait_recv()

        @pl.when(j >= relayed)
        def _():
            far_copy(j).wait_recv()

        total = (
            out_mixed[0, :, lanes(j)] + weight_near * near[j].astype(f32) + weight_far * far[j].astype(f32)
        )
        out_mixed[0, :, lanes(j)] = total
        out_params[0, :, lanes(j)] = out_params[0, :, lanes(j)] + mixing_rate * (
            total - out_estimate[0, :, lanes(j)]
        )

    def head(j):
        for way in (0, 1):
            for half in (0, 1):
                @pl.when(place[way] == 0)
                def _(way=way, half=half):
                    pass_on(way, 0, jnp.int32(2 * j + half), half)

    with jax.named_scope("lead"):
        grad_copy(0).wait()
        load_block(lead * 2 + other, 0).wait()
        turn(lead * 2 + other)
        give[0, lead_which] = product(lead, other, 0)
    with jax.named_scope("barrier"):
        pl.semaphore_wait(barrier, greeted)
        half_copy(0, lead_which).start()
    with jax.named_scope("lead2"):
        load_block(lead * 2 + core, 1).wait()
        turn(lead * 2 + core)
        keep_half(lead, lead_which, 0)
        half_copy(0, lead_which).wait_recv()
        head(0)
    with jax.named_scope("lead3"):
        grad_copy(1).wait()
        give_half(lead, lead_which, 1)
        keep_half(lead, lead_which, 1)
        for block in range(2, members - 2):
            load_block(block, 4).start()
        for k in range(2, len(bounds) - 1):
            grad_copy(k).start()
    with jax.named_scope("trail"):
        load_block(trail * 2 + other, 2).wait()
        turn(trail * 2 + other)
        for j in (0, 1):
            give_half(trail, 1 - lead_which, j)
        half_copy(1, lead_which).wait_recv()
        head(1)
        load_block(trail * 2 + core, 3).wait()
        turn(trail * 2 + core)
        for j in (0, 1):
            keep_half(trail, 1 - lead_which, j)
        for copy in loads:
            copy.start()
        for j in (0, 1):
            half_copy(j, 1 - lead_which).wait_recv()

    def turn_four(b):
        if members > 4:
            @pl.when(b == 1)
            def _():
                pltpu.make_async_copy(
                    act_v.at[pl.ds(2, members - 4)], act_v.at[pl.ds(2, members - 4)], act_sem.at[4]
                ).wait()

            for parity in (0, 1):
                for dest in (b, chips - 1 - b):
                    turn(dest * 2 + parity)

    def body(d, carry):
        for half in (0, 1):
            r = 2 * d + half
            for s in range(steps):
                odd_half = (half - begin[s]) % 2
                with jax.named_scope(f"pass{s}"):
                    if s < pairs and odd_half == 0:
                        guarded(
                            functools.partial(exchanged, s),
                            (r - begin[s]) // 2, chunks // 2, 0 if s else SPLIT,
                        )
                    for way in (0, 1):
                        least = 0 if s else jnp.where(place[way] == 0, 2 * SPLIT, 0)
                        pass_on(way, s, r - LAG * place[way] - begin[s], odd_half, least)
                if half == 0 and s == 0:
                    with jax.named_scope("turn"):
                        guarded(turn_four, d, pairs, 1)
                if half == 0 and s < pairs:
                    with jax.named_scope(f"mult{s}"):
                        guarded(
                            functools.partial(multiply, s), d - s - 1 if s else d + 1, chunks // 2
                        )
            with jax.named_scope("compress"):
                guarded(functools.partial(compress, half), r - first, chunks)
            with jax.named_scope("forward"):
                guarded(forward, r - first - RELAY, chunks)
            with jax.named_scope("finish"):
                guarded(finish, r - first - GOSSIP, chunks)
        return carry

    lax.fori_loop(1, (chunks + last + GOSSIP + 1) // 2, body, 0)

    with jax.named_scope("drain"):
        to_sibling((), half_r.at[0, 0]).wait_send()
        for way in (0, 1):
            for s in range(steps):
                @pl.when(steps - s > place[way])
                def _(way=way, s=s):
                    for k in range(DEPTH):
                        line_copy(way, s, chunks - 1 - k).wait_send()
        to_group(own, near, near_to, near_s, near_r.at[0], ()).wait_send()
        to_group(own, far, far_to, far_s, far_r.at[0], ()).wait_send()


def flush(pieces, *refs):
    sources, targets, sems = refs[:3], refs[3:6], refs[6]
    rows = sources[0].shape[1] // pieces
    copies = [
        pltpu.make_async_copy(
            sources[a].at[:, pl.ds(k * rows, rows)], targets[a].at[:, pl.ds(k * rows, rows)], sems.at[a, k]
        )
        for k in range(pieces)
        for a in range(3)
    ]
    for copy in copies:
        copy.start()
    for copy in copies:
        copy.wait()


def on_device(members, groups, params, estimate, mixed, acts, grads, exponents, edges):
    rows, width = params.shape[1:]
    tokens = acts.shape[0]
    chunks = CHUNKS
    cols = width // chunks
    chips = members // 2
    items = chips // 2 * chunks // 2
    slots = (chips - 1) * chunks
    ring = min(chunks, LAG * (chips - 1) + 2)
    span = RING if groups <= 4 else chunks
    factor = step_size / math.sqrt(members * tokens)
    cfg = (members, groups, chunks, rows, width, tokens, factor)
    wide = (chunks, rows, cols)
    tall = (items, 2, rows, 2 * cols)
    dma = pltpu.SemaphoreType.DMA
    any_spec = pl.BlockSpec(memory_space=pl.ANY)
    smem = pl.BlockSpec(memory_space=pltpu.SMEM)
    vmem = pl.BlockSpec(memory_space=pltpu.VMEM)
    results = pl.pallas_call(
        functools.partial(kernel, cfg),
        out_shape=[pltpu.VMEM(params.shape, f32)] * 3,
        in_specs=[any_spec] * 5 + [smem] * 2,
        out_specs=[vmem] * 3,
        scratch_shapes=[
            pltpu.VMEM((members, tokens, rows), bf16),
            pltpu.VMEM((members, rows, tokens), bf16),
            pltpu.VMEM((tokens, width), bf16),
            *[pltpu.VMEM((rows, width), f32)] * 3,
            *[pltpu.VMEM(tall, bf16)] * 3,
            pltpu.VMEM((2, slots, rows, cols), bf16),
            pltpu.VMEM((2, slots + chunks, rows, cols), bf16),
            *[pltpu.VMEM(wide, bf16)] * 3,
            dma((5,)), dma((chunks.bit_length(),)), dma((3,)),
            dma, dma((SPLIT, 2)), dma((chips // 2, SLOTS)),
            dma((2, chips - 1, DEPTH)), dma((2, chips - 1, ring)),
            dma, dma((span,)), dma, dma((span + DIRECT,)),
        ],
        compiler_params=pltpu.CompilerParams(
            collective_id=0, has_side_effects=True, vmem_limit_bytes=53 * 1024 * 1024
        ),
    )(params, estimate, mixed, acts, grads, exponents, edges)
    pieces = math.gcd(PIECES, rows // 8)
    return pl.pallas_call(
        functools.partial(flush, pieces),
        out_shape=[jax.ShapeDtypeStruct(params.shape, f32)] * 3,
        in_specs=[vmem] * 3,
        out_specs=[any_spec] * 3,
        scratch_shapes=[dma((3, pieces))],
        compiler_params=pltpu.CompilerParams(vmem_limit_bytes=1024 * 1024),
    )(*results)


def solution(mesh):
    shard = P("grp", "mem", None)
    tokens = P(("grp", "mem"), None)
    return jax.shard_map(
        functools.partial(on_device, mesh.shape["mem"], mesh.shape["grp"]),
        mesh=mesh,
        in_specs=(shard, shard, shard, tokens, tokens, P("grp", "mem"), P()),
        out_specs=(shard, shard, shard),
        check_vma=False,
    )
```

```python
import functools
import math

import jax
import jax.numpy as jnp
from jax import lax
from jax.experimental import pallas as pl
from jax.experimental.pallas import tpu as pltpu
from jax.sharding import PartitionSpec as P

step_size = 0.5
mixing_rate = 0.4
CHUNKS = 16
LAG = 1
RELAY = 1
GOSSIP = 3
DIRECT = 1
PIECES = 4
SLOTS = 4
RING = 8
MESH = pl.DeviceIdType.MESH
f32 = jnp.float32
bf16 = jnp.bfloat16


def kernel(
    cfg,
    params, estimate, mixed, acts, grads, exponents, edges,
    out_params, out_estimate, out_mixed,
    act_v, act_t, grad_v, par_v, est_v, mix_v,
    mine, give, got, line_out, line_in, own, near, far,
    act_sem, grad_sem, load_sem,
    pair_s, half_r, pair_r, line_s, line_r, near_s, near_r, far_s, far_r,
):
    members, groups, chunks, rows, width, tokens, factor = cfg
    chips = members // 2
    pairs = chips // 2
    steps = chips - 1
    cols = width // chunks
    g = lax.axis_index("grp")
    m = lax.axis_index("mem")
    chip, core = m // 2, m % 2
    other = 1 - core
    sibling = chip * 2 + other
    upper = jnp.where(chip < pairs, 0, 1)
    edge = jnp.where(chip < pairs, chip, chips - 1 - chip)
    inward = lax.rem(chip + chips + 1 - 2 * upper, chips) * 2 + core
    outward = lax.rem(chip + chips - 1 + 2 * upper, chips) * 2 + core
    ways = ((upper, edge, inward), (1 - upper, chips - 1 - edge, outward))
    odd = g % 2
    near_to = lax.rem(g + groups + 1 - 2 * odd, groups)
    far_to = lax.rem(g + groups - 1 + 2 * odd, groups)
    onward = lax.rem(g + groups + 2 - 4 * odd, groups)
    backward = lax.rem(g + groups - 2 + 4 * odd, groups)

    begin = [2 * s for s in range(pairs)]
    for s in range(pairs, steps):
        begin.append(begin[-1] + 1)
    first = max(begin[steps - p] + LAG * p for p in range(1, chips))
    first += first % 2

    def load_block(block, sem):
        return pltpu.make_async_copy(
            acts.at[:, pl.ds(pl.multiple_of(block * rows, rows), rows)], act_v.at[block], act_sem.at[sem]
        )

    def lanes(j):
        return pl.ds(pl.multiple_of(j * cols, cols), cols)

    bounds = [0, 2]
    while bounds[-1] < chunks:
        bounds.append(min(2 * bounds[-1], chunks))

    def grad_copy(k):
        at = pl.ds(bounds[k] * cols, (bounds[k + 1] - bounds[k]) * cols)
        return pltpu.make_async_copy(grads.at[:, at], grad_v.at[:, at], grad_sem.at[k])

    loads = [
        pltpu.make_async_copy(src.at[0], dst, load_sem.at[k])
        for k, (src, dst) in enumerate(((params, par_v), (estimate, est_v), (mixed, mix_v)))
    ]

    def to_sibling(at, recv_sem):
        return pltpu.make_async_remote_copy(
            src_ref=give.at[at] if at else give, dst_ref=got.at[at] if at else got,
            send_sem=pair_s, recv_sem=recv_sem,
            device_id={"mem": sibling}, device_id_type=MESH,
        )

    half_at = (0, 1, chunks // 2)
    half_of_width = (0, 1, 0)

    def half_copy(h, which):
        return to_sibling((half_at[h], which), half_r.at[h, which])

    def pair_copy(b, j):
        return to_sibling((b * (chunks // 2) + j,), pair_r.at[b, j % SLOTS])

    ring = line_r.shape[2]

    def line_copy(way, s, j):
        return pltpu.make_async_remote_copy(
            src_ref=line_out.at[way[0], s * chunks + j], dst_ref=line_in.at[way[0], s * chunks + j],
            send_sem=line_s.at[way[0], s, jnp.where(way[1] == 0, j % 2, 0)], recv_sem=line_r.at[way[0], s, j % ring],
            device_id={"mem": way[2]}, device_id_type=MESH,
        )

    def to_group(src, dst, peer, send_sem, recv_sem, at):
        return pltpu.make_async_remote_copy(
            src_ref=src.at[at] if at else src, dst_ref=dst.at[at] if at else dst,
            send_sem=send_sem, recv_sem=recv_sem,
            device_id={"grp": peer}, device_id_type=MESH,
        )

    span = near_r.shape[0]
    relayed = chunks - DIRECT

    def near_copy(j):
        return to_group(own, near, near_to, near_s, near_r.at[j % span], (j,))

    def relay_copy(j):
        return to_group(near, far, onward, far_s, far_r.at[j % span], (j,))

    def far_copy(j):
        return to_group(own, far, far_to, far_s, far_r.at[span + j - relayed], (j,))

    def guarded(run, j, count, least=0):
        @pl.when(jnp.logical_and(j >= least, j < count))
        def _():
            run(j)

    lead_which = 1 - upper
    lead = jnp.where(chip < pairs, chips - 1, 0)
    trail = chips - 1 - lead
    lead_next = jnp.where(chip < pairs, chips - 2, 1)
    trail_next = chips - 1 - lead_next

    grad_copy(0).start()
    load_block(lead * 2 + other, 0).start()

    barrier = pltpu.get_barrier_semaphore()
    for peer in ({"mem": sibling}, {"grp": near_to}, {"grp": far_to}, {"grp": onward}, {"grp": backward}):
        pl.semaphore_signal(barrier, inc=1, device_id=peer, device_id_type=MESH)
    pl.semaphore_signal(barrier, inc=1, device_id={"mem": inward}, device_id_type=MESH)

    @pl.when(edge > 0)
    def _():
        pl.semaphore_signal(barrier, inc=1, device_id={"mem": outward}, device_id_type=MESH)

    greeted = 7 - jnp.where(edge == 0, 1, 0)
    load_block(lead * 2 + core, 1).start()
    grad_copy(1).start()
    for parity, sem in ((other, 2), (core, 3)):
        load_block(lead_next * 2 + parity, sem).start()
    for parity, sem in ((other, 4), (core, 5)):
        for dest in (trail, trail_next):
            load_block(dest * 2 + parity, sem).start()

    def turn(block):
        act_t[block] = act_v[block].T

    def product(dest, parity, j):
        return jnp.dot(
            act_t[dest * 2 + parity],
            grad_v[:, pl.ds(pl.multiple_of(2 * j * cols, 2 * cols), 2 * cols)],
            preferred_element_type=f32,
        ).astype(bf16)

    def put(ref, i, which, value):
        for half in (0, 1):
            ref[i, which, half] = value[:, half * cols : (half + 1) * cols]

    def give_half(dest, which, h):
        put(give, half_at[h], which, product(dest, other, half_of_width[h]))
        half_copy(h, which).start()

    def keep_half(dest, which, h):
        put(mine, half_at[h], which, product(dest, core, half_of_width[h]))

    def multiply(b, j):
        i = b * (chunks // 2) + j
        if b == 0:
            for k in range(len(bounds) - 1):
                @pl.when(2 * j == bounds[k])
                def _(k=k):
                    grad_copy(k).wait()
        for which, dest in ((0, b), (1, chips - 1 - b)):
            put(give, i, which, product(dest, other, j))
        pair_copy(b, j).start()
        for which, dest in ((0, b), (1, chips - 1 - b)):
            put(mine, i, which, product(dest, core, j))

    def exchanged(b, j):
        pair_copy(b, j).wait_recv()

    def pair_sum(i, which, half):
        return mine[i, which, half].astype(f32) + got[i, which, half].astype(f32)

    def pass_on(way, s, j, least=0):
        far_dest = steps - s
        b = min(s, steps - s)
        which = 1 - way[0] if far_dest >= pairs else way[0]
        i = b * (chunks // 2) + j // 2
        slot = s * chunks + j

        @pl.when(jnp.logical_and(far_dest > way[1], jnp.logical_and(j >= least, j < chunks)))
        def _():
            @pl.when(way[1] == 0)
            def _():
                line_out[way[0], slot] = pair_sum(i, which, j % 2).astype(bf16)

            @pl.when(way[1] > 0)
            def _():
                line_copy(way, s, j).wait_recv()
                line_out[way[0], slot] = (
                    pair_sum(i, which, j % 2) + line_in[way[0], slot].astype(f32)
                ).astype(bf16)

            line_copy(way, s, j).start()

    def sent(s, j):
        line_copy(ways[0], s, j).wait_send()

    def pace(s, r):
        j = r - begin[s]

        @pl.when(jnp.logical_and(r > (4 if s == 0 else 3), jnp.logical_and(j >= 1, j < chunks)))
        def _():
            sent(s, j - 1)

        early = {0: ((4, 1, 0),), 1: ((2, 0, 1), (3, 0, 2)), 2: ((3, 0, 3),)}.get(s, ())
        for at, step, chunk in early:
            @pl.when(r == at)
            def _(step=step, chunk=chunk):
                sent(step, chunk)

    weight_right = edges[g]
    weight_left = edges[lax.rem(g + groups - 1, groups)]
    weight_self = 1.0 - weight_left - weight_right
    weight_near = jnp.where(odd == 1, weight_left, weight_right)
    weight_far = jnp.where(odd == 1, weight_right, weight_left)
    blocks = exponents.shape[1]
    block_rows = rows // blocks

    def compress(j):
        slot_of = [(steps - way[1]) * chunks + j for way in ways]

        @pl.when(j == 0)
        def _():
            for copy in loads:
                copy.wait()

        line_copy(ways[1], steps - ways[1][1], j).wait_recv()

        @pl.when(edge == 0)
        def _():
            line_in[upper, slot_of[0]] = jnp.zeros((rows, cols), bf16)

        @pl.when(edge > 0)
        def _():
            line_copy(ways[0], steps - edge, j).wait_recv()

        i = edge * (chunks // 2) + j // 2
        for b in range(blocks):
            exponent = exponents[0, b]
            scale = (jnp.int32(1) << exponent).astype(f32)
            inverse = (jnp.int32(1) << (15 - exponent)).astype(f32) * (2.0 ** -15)
            at = pl.ds(b * block_rows, block_rows)
            gradient = (
                mine[i, upper, j % 2, at, :].astype(f32)
                + got[i, upper, j % 2, at, :].astype(f32)
                + line_in[upper, slot_of[0], at, :].astype(f32)
                + line_in[1 - upper, slot_of[1], at, :].astype(f32)
            )
            stepped = par_v[at, lanes(j)] - factor * gradient
            levels = jnp.clip((stepped - est_v[at, lanes(j)]) * inverse, -1.0, 1.0).astype(bf16)
            own[j, at, :] = (levels.astype(f32) * scale).astype(bf16)
            out_params[0, at, lanes(j)] = stepped
        @pl.when(j >= relayed)
        def _():
            far_copy(j).start()

        near_copy(j).start()
        compressed = own[j].astype(f32)
        out_estimate[0, :, lanes(j)] = est_v[:, lanes(j)] + compressed
        out_mixed[0, :, lanes(j)] = mix_v[:, lanes(j)] + weight_self * compressed

    def forward(j):
        near_copy(j).wait_recv()

        @pl.when(j < relayed)
        def _():
            relay_copy(j).start()

    def finish(j):
        @pl.when(j < relayed)
        def _():
            relay_copy(j).wait_recv()

        @pl.when(j >= relayed)
        def _():
            far_copy(j).wait_recv()

        total = (
            out_mixed[0, :, lanes(j)] + weight_near * near[j].astype(f32) + weight_far * far[j].astype(f32)
        )
        out_mixed[0, :, lanes(j)] = total
        out_params[0, :, lanes(j)] = out_params[0, :, lanes(j)] + mixing_rate * (
            total - out_estimate[0, :, lanes(j)]
        )

    def head(s, j):
        @pl.when(edge == 0)
        def _():
            for half in (0, 1):
                if j == 1 and half == 0:
                    sent(0, 0)
                pass_on(ways[0], s, jnp.int32(2 * j + half))

    with jax.named_scope("lead"):
        grad_copy(0).wait()
        load_block(lead * 2 + other, 0).wait()
    with jax.named_scope("lead1"):
        turn(lead * 2 + other)
        put(give, 0, lead_which, product(lead, other, 0))
    with jax.named_scope("barrier"):
        pl.semaphore_wait(barrier, greeted)
        half_copy(0, lead_which).start()
    with jax.named_scope("lead2"):
        load_block(lead * 2 + core, 1).wait()
        turn(lead * 2 + core)
        keep_half(lead, lead_which, 0)
        half_copy(0, lead_which).wait_recv()
        head(0, 0)
    with jax.named_scope("lead3"):
        grad_copy(1).wait()
        give_half(lead, lead_which, 1)
        keep_half(lead, lead_which, 1)
        load_block(lead_next * 2 + other, 2).wait()
        turn(lead_next * 2 + other)
        give_half(lead_next, lead_which, 2)
        load_block(lead_next * 2 + core, 3).wait()
        turn(lead_next * 2 + core)
        keep_half(lead_next, lead_which, 2)
        for block in range(4, members - 4):
            load_block(block, 6).start()
        for k in range(2, len(bounds) - 1):
            grad_copy(k).start()

    def both_trails(parity, sem):
        block = act_v.at[pl.ds(0, 2)]
        pltpu.make_async_copy(block, block, act_sem.at[sem]).wait()
        turn(trail * 2 + parity)
        turn(trail_next * 2 + parity)

    with jax.named_scope("trail"):
        both_trails(other, 4)
        give_half(trail, 1 - lead_which, 0)
        half_copy(1, lead_which).wait_recv()
        head(0, 1)
        give_half(trail, 1 - lead_which, 1)
        give_half(trail_next, 1 - lead_which, 2)
    with jax.named_scope("trail2"):
        both_trails(core, 5)
        for h, dest in enumerate((trail, trail, trail_next)):
            keep_half(dest, 1 - lead_which, h)
        for copy in loads:
            copy.start()
        half_copy(2, lead_which).wait_recv()
        head(1, 0)
        for h in range(3):
            half_copy(h, 1 - lead_which).wait_recv()

    def turn_four(b):
        if members > 8:
            @pl.when(b == 2)
            def _():
                block = act_v.at[pl.ds(4, members - 8)]
                pltpu.make_async_copy(block, block, act_sem.at[6]).wait()

            for parity in (0, 1):
                for dest in (b, chips - 1 - b):
                    turn(dest * 2 + parity)

    sent_early = (4, 2)
    ready = [2, 1] + [0] * pairs

    def body(d, carry):
        for half in (0, 1):
            r = 2 * d + half
            for s in range(steps):
                odd_half = (half - begin[s]) % 2
                with jax.named_scope(f"pass{s}"):
                    if s < pairs and odd_half == 0:
                        guarded(
                            functools.partial(exchanged, s),
                            (r - begin[s]) // 2, chunks // 2, ready[s],
                        )
                    @pl.when(edge == 0)
                    def _(s=s, r=r):
                        pace(s, r)

                    for way in ways:
                        least = jnp.where(way[1] == 0, sent_early[s], 0) if s < 2 else 0
                        pass_on(way, s, r - LAG * way[1] - begin[s], least)
                if half == 0 and s == 0 and pairs > 2:
                    guarded(turn_four, d + 1, pairs, 2)
                if half == 0 and s < pairs:
                    with jax.named_scope(f"mult{s}"):
                        guarded(functools.partial(multiply, s), d + 1 - s, chunks // 2, ready[s])
            with jax.named_scope("compress"):
                guarded(compress, r - first, chunks)
            with jax.named_scope("forward"):
                guarded(forward, r - first - RELAY, chunks)
            with jax.named_scope("finish"):
                guarded(finish, r - first - GOSSIP, chunks)
        return carry

    lax.fori_loop(0, (chunks + first + GOSSIP + 1) // 2, body, 0)

    with jax.named_scope("drain"):
        to_sibling((), half_r.at[0, 0]).wait_send()
        for way in ways:
            for s in range(steps):
                @pl.when(jnp.logical_and(way[1] > 0, steps - s > way[1]))
                def _(way=way, s=s):
                    whole = line_out.at[way[0], pl.ds(s * chunks, chunks)]
                    pltpu.make_async_remote_copy(
                        src_ref=whole, dst_ref=whole, send_sem=line_s.at[way[0], s, 0],
                        recv_sem=line_r.at[way[0], s, 0],
                        device_id={"mem": way[2]}, device_id_type=MESH,
                    ).wait_send()

        @pl.when(edge == 0)
        def _():
            for s in range(steps):
                sent(s, chunks - 1)

        to_group(own, near, near_to, near_s, near_r.at[0], ()).wait_send()
        to_group(own, far, far_to, far_s, far_r.at[0], ()).wait_send()


def flush(pieces, *refs):
    sources, targets, sems = refs[:3], refs[3:6], refs[6]
    rows = sources[0].shape[1] // pieces
    copies = [
        pltpu.make_async_copy(
            sources[a].at[:, pl.ds(k * rows, rows)], targets[a].at[:, pl.ds(k * rows, rows)], sems.at[a, k]
        )
        for k in range(pieces)
        for a in range(3)
    ]
    for copy in copies:
        copy.start()
    for copy in copies:
        copy.wait()


def on_device(members, groups, params, estimate, mixed, acts, grads, exponents, edges):
    rows, width = params.shape[1:]
    tokens = acts.shape[0]
    chunks = CHUNKS
    cols = width // chunks
    chips = members // 2
    items = chips // 2 * chunks // 2
    slots = (chips - 1) * chunks
    ring = 6 if chips <= 4 else chunks
    span = RING if groups <= 4 else chunks
    factor = step_size / math.sqrt(members * tokens)
    cfg = (members, groups, chunks, rows, width, tokens, factor)
    wide = (chunks, rows, cols)
    tall = (items, 2, 2, rows, cols)
    dma = pltpu.SemaphoreType.DMA
    any_spec = pl.BlockSpec(memory_space=pl.ANY)
    smem = pl.BlockSpec(memory_space=pltpu.SMEM)
    vmem = pl.BlockSpec(memory_space=pltpu.VMEM)
    results = pl.pallas_call(
        functools.partial(kernel, cfg),
        out_shape=[pltpu.VMEM(params.shape, f32)] * 3,
        in_specs=[any_spec] * 5 + [smem] * 2,
        out_specs=[vmem] * 3,
        scratch_shapes=[
            pltpu.VMEM((members, tokens, rows), bf16),
            pltpu.VMEM((members, rows, tokens), bf16),
            pltpu.VMEM((tokens, width), bf16),
            *[pltpu.VMEM((rows, width), f32)] * 3,
            *[pltpu.VMEM(tall, bf16)] * 3,
            pltpu.VMEM((2, slots, rows, cols), bf16),
            pltpu.VMEM((2, slots + chunks, rows, cols), bf16),
            *[pltpu.VMEM(wide, bf16)] * 3,
            dma((7,)), dma((chunks.bit_length(),)), dma((3,)),
            dma, dma((3, 2)), dma((chips // 2, SLOTS)),
            dma((2, chips - 1, 2)), dma((2, chips - 1, ring)),
            dma, dma((span,)), dma, dma((span + DIRECT,)),
        ],
        compiler_params=pltpu.CompilerParams(
            collective_id=0, has_side_effects=True, vmem_limit_bytes=53 * 1024 * 1024
        ),
    )(params, estimate, mixed, acts, grads, exponents, edges)
    pieces = math.gcd(PIECES, rows // 8)
    return pl.pallas_call(
        functools.partial(flush, pieces),
        out_shape=[jax.ShapeDtypeStruct(params.shape, f32)] * 3,
        in_specs=[vmem] * 3,
        out_specs=[any_spec] * 3,
        scratch_shapes=[dma((3, pieces))],
        compiler_params=pltpu.CompilerParams(vmem_limit_bytes=1024 * 1024),
    )(*results)


def solution(mesh):
    shard = P("grp", "mem", None)
    tokens = P(("grp", "mem"), None)
    return jax.shard_map(
        functools.partial(on_device, mesh.shape["mem"], mesh.shape["grp"]),
        mesh=mesh,
        in_specs=(shard, shard, shard, tokens, tokens, P("grp", "mem"), P()),
        out_specs=(shard, shard, shard),
        check_vma=False,
    )
```

```python
import functools
import math

import jax
import jax.numpy as jnp
from jax import lax
from jax.experimental import pallas as pl
from jax.experimental.pallas import tpu as pltpu
from jax.sharding import PartitionSpec as P

step_size = 0.5
mixing_rate = 0.4
CHUNKS = 16
LAG = 1
RELAY = 1
GOSSIP = 2
DIRECT = 1
PIECES = 4
SLOTS = 2
STEP = 1
RING = 6
PARTS = 2
MESH = pl.DeviceIdType.MESH
f32 = jnp.float32
bf16 = jnp.bfloat16


def kernel(
    cfg,
    params, estimate, mixed, acts, grads, exponents, edges,
    out_params, out_estimate, out_mixed,
    act_v, act_t, grad_v, par_v, est_v, mix_v,
    mine, give, got, line_out, line_in, own, near, far,
    act_sem, grad_sem, load_sem,
    pair_s, half_r, pair_r, line_s, line_r, near_s, near_r, far_s, far_r,
):
    members, groups, chunks, rows, width, tokens, factor = cfg
    chips = members // 2
    pairs = chips // 2
    steps = chips - 1
    cols = width // chunks
    g = lax.axis_index("grp")
    m = lax.axis_index("mem")
    chip, core = m // 2, m % 2
    other = 1 - core
    sibling = chip * 2 + other
    upper = jnp.where(chip < pairs, 0, 1)
    edge = jnp.where(chip < pairs, chip, chips - 1 - chip)
    inward = lax.rem(chip + chips + 1 - 2 * upper, chips) * 2 + core
    outward = lax.rem(chip + chips - 1 + 2 * upper, chips) * 2 + core
    ways = ((upper, edge, inward), (1 - upper, chips - 1 - edge, outward))
    odd = g % 2
    near_to = lax.rem(g + groups + 1 - 2 * odd, groups)
    far_to = lax.rem(g + groups - 1 + 2 * odd, groups)
    onward = lax.rem(g + groups + 2 - 4 * odd, groups)
    backward = lax.rem(g + groups - 2 + 4 * odd, groups)

    begin = [2 * s for s in range(pairs)]
    for s in range(pairs, steps):
        begin.append(begin[-1] + STEP)
    first = max(begin[steps - p] + LAG * p for p in range(1, chips))

    def load_block(block, sem):
        return pltpu.make_async_copy(
            acts.at[:, pl.ds(pl.multiple_of(block * rows, rows), rows)], act_v.at[block], act_sem.at[sem]
        )

    def lanes(j):
        return pl.ds(pl.multiple_of(j * cols, cols), cols)

    bounds = [0, 2]
    while bounds[-1] < chunks:
        bounds.append(min(2 * bounds[-1], chunks))

    def grad_copy(k):
        at = pl.ds(bounds[k] * cols, (bounds[k + 1] - bounds[k]) * cols)
        return pltpu.make_async_copy(grads.at[:, at], grad_v.at[:, at], grad_sem.at[k])

    loads = [
        pltpu.make_async_copy(src.at[0], dst, load_sem.at[k])
        for k, (src, dst) in enumerate(((params, par_v), (estimate, est_v), (mixed, mix_v)))
    ]

    def to_sibling(at, recv_sem):
        return pltpu.make_async_remote_copy(
            src_ref=give.at[at] if at else give, dst_ref=got.at[at] if at else got,
            send_sem=pair_s, recv_sem=recv_sem,
            device_id={"mem": sibling}, device_id_type=MESH,
        )

    half_at = (0, 1, chunks // 2)
    half_of_width = (0, 1, 0)

    def half_copy(h, which):
        return to_sibling((half_at[h], which), half_r.at[h, which])

    def pair_copy(b, j):
        return to_sibling((b * (chunks // 2) + j,), pair_r.at[b, j % SLOTS])

    ring = line_r.shape[2]

    def line_copy(way, s, j):
        return pltpu.make_async_remote_copy(
            src_ref=line_out.at[way[0], s * chunks + j], dst_ref=line_in.at[way[0], s * chunks + j],
            send_sem=line_s.at[way[0], s, jnp.where(way[1] == 0, j % 2, 0)], recv_sem=line_r.at[way[0], s, j % ring],
            device_id={"mem": way[2]}, device_id_type=MESH,
        )

    def to_group(src, dst, peer, send_sem, recv_sem, at):
        return pltpu.make_async_remote_copy(
            src_ref=src.at[at] if at else src, dst_ref=dst.at[at] if at else dst,
            send_sem=send_sem, recv_sem=recv_sem,
            device_id={"grp": peer}, device_id_type=MESH,
        )

    span = near_r.shape[0]
    relayed = chunks - DIRECT

    def part_of(j, k):
        return (j, pl.ds(k * (rows // PARTS), rows // PARTS))

    def near_copy(j, k):
        return to_group(own, near, near_to, near_s, near_r.at[j % span, k], part_of(j, k))

    def relay_copy(j, k):
        return to_group(near, far, onward, far_s, far_r.at[j % span, k], part_of(j, k))

    def far_copy(j):
        return to_group(own, far, far_to, far_s, far_r.at[span + j - relayed, 0], (j,))

    def guarded(run, j, count, least=0):
        @pl.when(jnp.logical_and(j >= least, j < count))
        def _():
            run(j)

    lead_which = 1 - upper
    lead = jnp.where(chip < pairs, chips - 1, 0)
    trail = chips - 1 - lead
    lead_next = jnp.where(chip < pairs, chips - 2, 1)
    trail_next = chips - 1 - lead_next

    grad_copy(0).start()
    load_block(lead * 2 + other, 0).start()

    barrier = pltpu.get_barrier_semaphore()
    for peer in ({"mem": sibling}, {"grp": near_to}, {"grp": far_to}, {"grp": onward}, {"grp": backward}):
        pl.semaphore_signal(barrier, inc=1, device_id=peer, device_id_type=MESH)
    pl.semaphore_signal(barrier, inc=1, device_id={"mem": inward}, device_id_type=MESH)

    @pl.when(edge > 0)
    def _():
        pl.semaphore_signal(barrier, inc=1, device_id={"mem": outward}, device_id_type=MESH)

    greeted = 7 - jnp.where(edge == 0, 1, 0)
    load_block(lead * 2 + core, 1).start()
    grad_copy(1).start()
    for parity, sem in ((other, 2), (core, 3)):
        load_block(lead_next * 2 + parity, sem).start()
    for parity, sem in ((other, 4), (core, 5)):
        for dest in (trail, trail_next):
            load_block(dest * 2 + parity, sem).start()

    def turn(block):
        act_t[block] = act_v[block].T

    def product(dest, parity, j):
        return jnp.dot(
            act_t[dest * 2 + parity],
            grad_v[:, pl.ds(pl.multiple_of(2 * j * cols, 2 * cols), 2 * cols)],
            preferred_element_type=f32,
        ).astype(bf16)

    def put(ref, i, which, value):
        for half in (0, 1):
            ref[i, which, half] = value[:, half * cols : (half + 1) * cols]

    def give_half(dest, which, h):
        put(give, half_at[h], which, product(dest, other, half_of_width[h]))
        half_copy(h, which).start()

    def keep_half(dest, which, h):
        put(mine, half_at[h], which, product(dest, core, half_of_width[h]))

    def multiply(b, j):
        i = b * (chunks // 2) + j
        if b == 0:
            for k in range(len(bounds) - 1):
                @pl.when(2 * j == bounds[k])
                def _(k=k):
                    grad_copy(k).wait()
        for which, dest in ((0, b), (1, chips - 1 - b)):
            put(give, i, which, product(dest, other, j))
        pair_copy(b, j).start()
        for which, dest in ((0, b), (1, chips - 1 - b)):
            put(mine, i, which, product(dest, core, j))

    def exchanged(b, j):
        pair_copy(b, j).wait_recv()

    def pair_sum(i, which, half):
        return mine[i, which, half].astype(f32) + got[i, which, half].astype(f32)

    def pass_on(way, s, j, least=0):
        far_dest = steps - s
        b = min(s, steps - s)
        which = 1 - way[0] if far_dest >= pairs else way[0]
        i = b * (chunks // 2) + j // 2
        slot = s * chunks + j

        @pl.when(jnp.logical_and(far_dest > way[1], jnp.logical_and(j >= least, j < chunks)))
        def _():
            @pl.when(way[1] == 0)
            def _():
                line_out[way[0], slot] = pair_sum(i, which, j % 2).astype(bf16)

            @pl.when(way[1] > 0)
            def _():
                line_copy(way, s, j).wait_recv()
                line_out[way[0], slot] = (
                    pair_sum(i, which, j % 2) + line_in[way[0], slot].astype(f32)
                ).astype(bf16)

            line_copy(way, s, j).start()

    def sent(s, j):
        line_copy(ways[0], s, j).wait_send()

    late = begin == [0, 2, 3]

    def pace(s, r):
        j = r - begin[s]

        @pl.when(jnp.logical_and(r > (4 if s == 0 else 3), jnp.logical_and(j >= 1, (r if late else j) < chunks)))
        def _():
            sent(s, j - 1)

        turns = {0: ((4, 1, 0),), 1: ((2, 0, 1), (3, 0, 2)), 2: ((3, 0, 3),)}.get(s, ())
        if late:
            turns += {
                1: ((chunks, 0, chunks - 1), (chunks + 1, 2, chunks - 4)),
                2: ((chunks, 1, chunks - 3), (chunks + 1, 1, chunks - 2), (chunks + 2, 2, chunks - 3)),
            }.get(s, ())
        for at, step, chunk in turns:
            @pl.when(r == at)
            def _(step=step, chunk=chunk):
                sent(step, chunk)

    weight_right = edges[g]
    weight_left = edges[lax.rem(g + groups - 1, groups)]
    weight_self = 1.0 - weight_left - weight_right
    weight_near = jnp.where(odd == 1, weight_left, weight_right)
    weight_far = jnp.where(odd == 1, weight_right, weight_left)
    blocks = exponents.shape[1]
    block_rows = rows // blocks

    def compress(j):
        slot_of = [(steps - way[1]) * chunks + j for way in ways]

        @pl.when(j == 0)
        def _():
            for copy in loads:
                copy.wait()

        line_copy(ways[1], steps - ways[1][1], j).wait_recv()

        @pl.when(edge == 0)
        def _():
            line_in[upper, slot_of[0]] = jnp.zeros((rows, cols), bf16)

        @pl.when(edge > 0)
        def _():
            line_copy(ways[0], steps - edge, j).wait_recv()

        i = edge * (chunks // 2) + j // 2
        for b in range(blocks):
            exponent = exponents[0, b]
            scale = (jnp.int32(1) << exponent).astype(f32)
            inverse = (jnp.int32(1) << (15 - exponent)).astype(f32) * (2.0 ** -15)
            at = pl.ds(b * block_rows, block_rows)
            gradient = (
                mine[i, upper, j % 2, at, :].astype(f32)
                + got[i, upper, j % 2, at, :].astype(f32)
                + line_in[upper, slot_of[0], at, :].astype(f32)
                + line_in[1 - upper, slot_of[1], at, :].astype(f32)
            )
            stepped = par_v[at, lanes(j)] - factor * gradient
            levels = jnp.clip((stepped - est_v[at, lanes(j)]) * inverse, -1.0, 1.0).astype(bf16)
            own[j, at, :] = (levels.astype(f32) * scale).astype(bf16)
            out_params[0, at, lanes(j)] = stepped
        @pl.when(j >= relayed)
        def _():
            far_copy(j).start()

        for k in range(PARTS):
            near_copy(j, k).start()
        compressed = own[j].astype(f32)
        out_estimate[0, :, lanes(j)] = est_v[:, lanes(j)] + compressed
        out_mixed[0, :, lanes(j)] = mix_v[:, lanes(j)] + weight_self * compressed

    def forward(j):
        for k in range(PARTS):
            near_copy(j, k).wait_recv()

            @pl.when(j < relayed)
            def _(k=k):
                relay_copy(j, k).start()

    def finish(j):
        @pl.when(j < relayed)
        def _():
            for k in range(PARTS):
                relay_copy(j, k).wait_recv()

        @pl.when(j >= relayed)
        def _():
            far_copy(j).wait_recv()

        total = (
            out_mixed[0, :, lanes(j)] + weight_near * near[j].astype(f32) + weight_far * far[j].astype(f32)
        )
        out_mixed[0, :, lanes(j)] = total
        out_params[0, :, lanes(j)] = out_params[0, :, lanes(j)] + mixing_rate * (
            total - out_estimate[0, :, lanes(j)]
        )

    def head(s, j):
        @pl.when(edge == 0)
        def _():
            for half in (0, 1):
                if j == 1 and half == 0:
                    sent(0, 0)
                pass_on(ways[0], s, jnp.int32(2 * j + half))

    with jax.named_scope("lead"):
        grad_copy(0).wait()
        load_block(lead * 2 + other, 0).wait()
    with jax.named_scope("lead1"):
        turn(lead * 2 + other)
        put(give, 0, lead_which, product(lead, other, 0))
    with jax.named_scope("barrier"):
        pl.semaphore_wait(barrier, greeted)
        half_copy(0, lead_which).start()
    with jax.named_scope("lead2"):
        load_block(lead * 2 + core, 1).wait()
        turn(lead * 2 + core)
        keep_half(lead, lead_which, 0)
        half_copy(0, lead_which).wait_recv()
        head(0, 0)
    with jax.named_scope("lead3"):
        grad_copy(1).wait()
        give_half(lead, lead_which, 1)
        keep_half(lead, lead_which, 1)
        load_block(lead_next * 2 + other, 2).wait()
        turn(lead_next * 2 + other)
        give_half(lead_next, lead_which, 2)
        load_block(lead_next * 2 + core, 3).wait()
        turn(lead_next * 2 + core)
        keep_half(lead_next, lead_which, 2)
        for block in range(4, members - 4):
            load_block(block, 6).start()
        for k in range(2, len(bounds) - 1):
            grad_copy(k).start()

    def both_trails(parity, sem):
        block = act_v.at[pl.ds(0, 2)]
        pltpu.make_async_copy(block, block, act_sem.at[sem]).wait()
        turn(trail * 2 + parity)
        turn(trail_next * 2 + parity)

    with jax.named_scope("trail"):
        both_trails(other, 4)
        give_half(trail, 1 - lead_which, 0)
        half_copy(1, lead_which).wait_recv()
        head(0, 1)
        give_half(trail, 1 - lead_which, 1)
        give_half(trail_next, 1 - lead_which, 2)
    with jax.named_scope("trail2"):
        both_trails(core, 5)
        for h, dest in enumerate((trail, trail, trail_next)):
            keep_half(dest, 1 - lead_which, h)
        for copy in loads:
            copy.start()
        half_copy(2, lead_which).wait_recv()
        head(1, 0)
        for h in range(3):
            half_copy(h, 1 - lead_which).wait_recv()

    def turn_four(b):
        if members > 8:
            @pl.when(b == 2)
            def _():
                block = act_v.at[pl.ds(4, members - 8)]
                pltpu.make_async_copy(block, block, act_sem.at[6]).wait()

            for parity in (0, 1):
                for dest in (b, chips - 1 - b):
                    turn(dest * 2 + parity)

    sent_early = (4, 2)
    ready = [2, 1] + [0] * pairs

    def body(d, carry):
        for half in (0, 1):
            r = 2 * d + half
            for s in range(steps):
                odd_half = (half - begin[s]) % 2
                with jax.named_scope(f"pass{s}"):
                    if s < pairs and odd_half == 0:
                        guarded(
                            functools.partial(exchanged, s),
                            (r - begin[s]) // 2, chunks // 2, ready[s],
                        )
                    @pl.when(edge == 0)
                    def _(s=s, r=r):
                        pace(s, r)

                    for way in ways:
                        least = jnp.where(way[1] == 0, sent_early[s], 0) if s < 2 else 0
                        pass_on(way, s, r - LAG * way[1] - begin[s], least)
                if half == 0 and s == 0 and pairs > 2:
                    guarded(turn_four, d + 1, pairs, 2)
                if half == 0 and s < pairs:
                    with jax.named_scope(f"mult{s}"):
                        guarded(functools.partial(multiply, s), d + 1 - s, chunks // 2, ready[s])
            with jax.named_scope("compress"):
                guarded(compress, r - first, chunks)
            with jax.named_scope("forward"):
                guarded(forward, r - first - RELAY, chunks)
            with jax.named_scope("finish"):
                guarded(finish, r - first - GOSSIP, chunks)
        return carry

    turns = (chunks + first + 1) // 2
    lax.fori_loop(0, turns, body, 0)

    with jax.named_scope("tail"):
        for t in range(2 * turns - first, chunks + max(RELAY, GOSSIP)):
            if 0 <= t - GOSSIP < chunks:
                finish(t - GOSSIP)
            if 0 <= t - RELAY < chunks:
                forward(t - RELAY)


    with jax.named_scope("drain"):
        to_sibling((), half_r.at[0, 0]).wait_send()
        for way in ways:
            for s in range(steps):
                @pl.when(jnp.logical_and(way[1] > 0, steps - s > way[1]))
                def _(way=way, s=s):
                    whole = line_out.at[way[0], pl.ds(s * chunks, chunks)]
                    pltpu.make_async_remote_copy(
                        src_ref=whole, dst_ref=whole, send_sem=line_s.at[way[0], s, 0],
                        recv_sem=line_r.at[way[0], s, 0],
                        device_id={"mem": way[2]}, device_id_type=MESH,
                    ).wait_send()

        @pl.when(edge == 0)
        def _():
            for s in range(1 if late else 0, steps):
                sent(s, chunks - 1)
            if late:
                sent(2, chunks - 2)

        to_group(own, near, near_to, near_s, near_r.at[0, 0], ()).wait_send()
        to_group(own, far, far_to, far_s, far_r.at[0, 0], ()).wait_send()


def flush(pieces, *refs):
    sources, targets, sems = refs[:3], refs[3:6], refs[6]
    rows = sources[0].shape[1] // pieces
    copies = [
        pltpu.make_async_copy(
            sources[a].at[:, pl.ds(k * rows, rows)], targets[a].at[:, pl.ds(k * rows, rows)], sems.at[a, k]
        )
        for k in range(pieces)
        for a in range(3)
    ]
    for copy in copies:
        copy.start()
    for copy in copies:
        copy.wait()


def on_device(members, groups, params, estimate, mixed, acts, grads, exponents, edges):
    rows, width = params.shape[1:]
    tokens = acts.shape[0]
    chunks = CHUNKS
    cols = width // chunks
    chips = members // 2
    items = chips // 2 * chunks // 2
    slots = (chips - 1) * chunks
    ring = 6 if chips <= 4 else chunks
    span = RING if groups <= 4 else chunks
    factor = step_size / math.sqrt(members * tokens)
    cfg = (members, groups, chunks, rows, width, tokens, factor)
    wide = (chunks, rows, cols)
    tall = (items, 2, 2, rows, cols)
    dma = pltpu.SemaphoreType.DMA
    any_spec = pl.BlockSpec(memory_space=pl.ANY)
    smem = pl.BlockSpec(memory_space=pltpu.SMEM)
    vmem = pl.BlockSpec(memory_space=pltpu.VMEM)
    results = pl.pallas_call(
        functools.partial(kernel, cfg),
        out_shape=[pltpu.VMEM(params.shape, f32)] * 3,
        in_specs=[any_spec] * 5 + [smem] * 2,
        out_specs=[vmem] * 3,
        scratch_shapes=[
            pltpu.VMEM((members, tokens, rows), bf16),
            pltpu.VMEM((members, rows, tokens), bf16),
            pltpu.VMEM((tokens, width), bf16),
            *[pltpu.VMEM((rows, width), f32)] * 3,
            *[pltpu.VMEM(tall, bf16)] * 3,
            pltpu.VMEM((2, slots, rows, cols), bf16),
            pltpu.VMEM((2, slots + chunks, rows, cols), bf16),
            *[pltpu.VMEM(wide, bf16)] * 3,
            dma((7,)), dma((chunks.bit_length(),)), dma((3,)),
            dma, dma((3, 2)), dma((chips // 2, SLOTS)),
            dma((2, chips - 1, 2)), dma((2, chips - 1, ring)),
            dma, dma((span, PARTS)), dma, dma((span + DIRECT, PARTS)),
        ],
        compiler_params=pltpu.CompilerParams(
            collective_id=0, has_side_effects=True, vmem_limit_bytes=53 * 1024 * 1024
        ),
    )(params, estimate, mixed, acts, grads, exponents, edges)
    pieces = math.gcd(PIECES, rows // 8)
    return pl.pallas_call(
        functools.partial(flush, pieces),
        out_shape=[jax.ShapeDtypeStruct(params.shape, f32)] * 3,
        in_specs=[vmem] * 3,
        out_specs=[any_spec] * 3,
        scratch_shapes=[dma((3, pieces))],
        compiler_params=pltpu.CompilerParams(vmem_limit_bytes=1024 * 1024),
    )(*results)


def solution(mesh):
    shard = P("grp", "mem", None)
    tokens = P(("grp", "mem"), None)
    return jax.shard_map(
        functools.partial(on_device, mesh.shape["mem"], mesh.shape["grp"]),
        mesh=mesh,
        in_specs=(shard, shard, shard, tokens, tokens, P("grp", "mem"), P()),
        out_specs=(shard, shard, shard),
        check_vma=False,
    )
```

```python
import functools
import math

import jax
import jax.numpy as jnp
from jax import lax
from jax.experimental import pallas as pl
from jax.experimental.pallas import tpu as pltpu
from jax.sharding import PartitionSpec as P

step_size = 0.5
mixing_rate = 0.4
CHUNKS = 16
LAG = 1
RELAY = 1
GOSSIP = 2
DIRECT = 1
PIECES = 4
SLOTS = 2
STEP = 1
RING = 5
PARTS = 2
MESH = pl.DeviceIdType.MESH
f32 = jnp.float32
bf16 = jnp.bfloat16


def kernel(
    cfg,
    params, estimate, mixed, acts, grads, exponents, edges,
    out_params, out_estimate, out_mixed,
    act_v, act_t, grad_v, par_v, est_v, mix_v,
    mine, give, got, line_out, line_in, own, near, far,
    act_sem, grad_sem, load_sem,
    pair_s, half_r, first_r, pair_r, line_s, line_r, near_s, near_r, far_s, far_r,
):
    members, groups, chunks, rows, width, tokens, factor = cfg
    chips = members // 2
    pairs = chips // 2
    steps = chips - 1
    cols = width // chunks
    g = lax.axis_index("grp")
    m = lax.axis_index("mem")
    chip, core = m // 2, m % 2
    other = 1 - core
    sibling = chip * 2 + other
    upper = jnp.where(chip < pairs, 0, 1)
    edge = jnp.where(chip < pairs, chip, chips - 1 - chip)
    inward = lax.rem(chip + chips + 1 - 2 * upper, chips) * 2 + core
    outward = lax.rem(chip + chips - 1 + 2 * upper, chips) * 2 + core
    ways = ((upper, edge, inward, 0), (1 - upper, chips - 1 - edge, outward, 1))
    odd = g % 2
    near_to = lax.rem(g + groups + 1 - 2 * odd, groups)
    far_to = lax.rem(g + groups - 1 + 2 * odd, groups)
    onward = lax.rem(g + groups + 2 - 4 * odd, groups)
    backward = lax.rem(g + groups - 2 + 4 * odd, groups)

    begin = [2 * s for s in range(pairs)]
    for s in range(pairs, steps):
        begin.append(begin[-1] + STEP)
    first = max(begin[steps - p] + LAG * p for p in range(1, chips))

    def load_block(block, sem):
        return pltpu.make_async_copy(
            acts.at[:, pl.ds(pl.multiple_of(block * rows, rows), rows)], act_v.at[block], act_sem.at[sem]
        )

    def lanes(j):
        return pl.ds(pl.multiple_of(j * cols, cols), cols)

    bounds = [0, 2]
    while bounds[-1] < chunks:
        bounds.append(min(2 * bounds[-1], chunks))

    def grad_copy(k):
        at = pl.ds(bounds[k] * cols, (bounds[k + 1] - bounds[k]) * cols)
        return pltpu.make_async_copy(grads.at[:, at], grad_v.at[:, at], grad_sem.at[k])

    loads = [
        pltpu.make_async_copy(src.at[0], dst, load_sem.at[k])
        for k, (src, dst) in enumerate(((params, par_v), (estimate, est_v), (mixed, mix_v)))
    ]

    def to_sibling(at, recv_sem):
        return pltpu.make_async_remote_copy(
            src_ref=give.at[at] if at else give, dst_ref=got.at[at] if at else got,
            send_sem=pair_s, recv_sem=recv_sem,
            device_id={"mem": sibling}, device_id_type=MESH,
        )

    half_at = (0, 1, chunks // 2)
    half_of_width = (0, 1, 0)

    def half_copy(h, which):
        return to_sibling((half_at[h], which), half_r.at[h, which])

    def first_copy(half):
        return to_sibling((0, lead_which, half), half_r.at[0, lead_which] if half == 0 else first_r)

    def pair_copy(b, j):
        return to_sibling((b * (chunks // 2) + j,), pair_r.at[b, j % SLOTS])

    ring = line_r.shape[2]

    def line_slot(way, s, j):
        if way[3]:
            return 2 * steps + jnp.minimum(s, pairs - 2)
        return 2 * s + jnp.where(way[1] == 0, j % 2, 0)

    def line_copy(way, s, j):
        return pltpu.make_async_remote_copy(
            src_ref=line_out.at[way[0], s * chunks + j], dst_ref=line_in.at[way[0], s * chunks + j],
            send_sem=line_s.at[line_slot(way, s, j)], recv_sem=line_r.at[way[0], s, j % ring],
            device_id={"mem": way[2]}, device_id_type=MESH,
        )

    def to_group(src, dst, peer, send_sem, recv_sem, at):
        return pltpu.make_async_remote_copy(
            src_ref=src.at[at] if at else src, dst_ref=dst.at[at] if at else dst,
            send_sem=send_sem, recv_sem=recv_sem,
            device_id={"grp": peer}, device_id_type=MESH,
        )

    span = near_r.shape[0]
    relayed = chunks - DIRECT

    def part_of(j, k):
        return (j, pl.ds(k * (rows // PARTS), rows // PARTS))

    def near_copy(j, k):
        return to_group(own, near, near_to, near_s, near_r.at[j % span, k], part_of(j, k))

    def relay_copy(j, k):
        return to_group(near, far, onward, far_s, far_r.at[j % span, k], part_of(j, k))

    def far_copy(j):
        return to_group(own, far, far_to, far_s, far_r.at[span + j - relayed, 0], (j,))

    def guarded(run, j, count, least=0):
        @pl.when(jnp.logical_and(j >= least, j < count))
        def _():
            run(j)

    lead_which = 1 - upper
    lead = jnp.where(chip < pairs, chips - 1, 0)
    trail = chips - 1 - lead
    lead_next = jnp.where(chip < pairs, chips - 2, 1)
    trail_next = chips - 1 - lead_next

    grad_copy(0).start()
    load_block(lead * 2 + other, 0).start()

    barrier = pltpu.get_barrier_semaphore()
    for peer in ({"mem": sibling}, {"grp": near_to}, {"grp": far_to}, {"grp": onward}, {"grp": backward}):
        pl.semaphore_signal(barrier, inc=1, device_id=peer, device_id_type=MESH)
    pl.semaphore_signal(barrier, inc=1, device_id={"mem": inward}, device_id_type=MESH)

    @pl.when(edge > 0)
    def _():
        pl.semaphore_signal(barrier, inc=1, device_id={"mem": outward}, device_id_type=MESH)

    greeted = 7 - jnp.where(edge == 0, 1, 0)
    load_block(lead * 2 + core, 1).start()
    grad_copy(1).start()
    for parity, sem in ((other, 2), (core, 3)):
        load_block(lead_next * 2 + parity, sem).start()
    for parity, sem in ((other, 4), (core, 5)):
        for dest in (trail, trail_next):
            load_block(dest * 2 + parity, sem).start()

    def turn(block):
        act_t[block] = act_v[block].T

    def product(dest, parity, j):
        return jnp.dot(
            act_t[dest * 2 + parity],
            grad_v[:, pl.ds(pl.multiple_of(2 * j * cols, 2 * cols), 2 * cols)],
            preferred_element_type=f32,
        ).astype(bf16)

    def put(ref, i, which, value):
        for half in (0, 1):
            ref[i, which, half] = value[:, half * cols : (half + 1) * cols]

    def give_half(dest, which, h):
        put(give, half_at[h], which, product(dest, other, half_of_width[h]))
        half_copy(h, which).start()

    def keep_half(dest, which, h):
        put(mine, half_at[h], which, product(dest, core, half_of_width[h]))

    def multiply(b, j):
        i = b * (chunks // 2) + j
        if b == 0:
            for k in range(len(bounds) - 1):
                @pl.when(2 * j == bounds[k])
                def _(k=k):
                    grad_copy(k).wait()
        for which, dest in ((0, b), (1, chips - 1 - b)):
            put(give, i, which, product(dest, other, j))
        pair_copy(b, j).start()
        for which, dest in ((0, b), (1, chips - 1 - b)):
            put(mine, i, which, product(dest, core, j))

    def exchanged(b, j):
        pair_copy(b, j).wait_recv()

    def pair_sum(i, which, half):
        return mine[i, which, half].astype(f32) + got[i, which, half].astype(f32)

    def pass_on(way, s, j, least=0):
        far_dest = steps - s
        b = min(s, steps - s)
        which = 1 - way[0] if far_dest >= pairs else way[0]
        i = b * (chunks // 2) + j // 2
        slot = s * chunks + j

        @pl.when(jnp.logical_and(far_dest > way[1], jnp.logical_and(j >= least, j < chunks)))
        def _():
            @pl.when(way[1] == 0)
            def _():
                line_out[way[0], slot] = pair_sum(i, which, j % 2).astype(bf16)

            @pl.when(way[1] > 0)
            def _():
                line_copy(way, s, j).wait_recv()
                line_out[way[0], slot] = (
                    pair_sum(i, which, j % 2) + line_in[way[0], slot].astype(f32)
                ).astype(bf16)

            line_copy(way, s, j).start()

    def sent(s, j):
        line_copy(ways[0], s, j).wait_send()

    late = begin == [0, 2, 3]

    def pace(s, r):
        j = r - begin[s]

        @pl.when(jnp.logical_and(r > (4 if s == 0 else 3), jnp.logical_and(j >= 1, (r if late else j) < chunks)))
        def _():
            sent(s, j - 1)

        turns = {0: ((4, 1, 0),), 1: ((2, 0, 1), (3, 0, 2)), 2: ((3, 0, 3),)}.get(s, ())
        if late:
            turns += {
                1: ((chunks, 0, chunks - 1), (chunks + 1, 2, chunks - 4)),
                2: ((chunks, 1, chunks - 3), (chunks + 1, 1, chunks - 2), (chunks + 2, 2, chunks - 3)),
            }.get(s, ())
        for at, step, chunk in turns:
            @pl.when(r == at)
            def _(step=step, chunk=chunk):
                sent(step, chunk)

    weight_right = edges[g]
    weight_left = edges[lax.rem(g + groups - 1, groups)]
    weight_self = 1.0 - weight_left - weight_right
    weight_near = jnp.where(odd == 1, weight_left, weight_right)
    weight_far = jnp.where(odd == 1, weight_right, weight_left)
    blocks = exponents.shape[1]
    block_rows = rows // blocks

    def compress(j):
        slot_of = [(steps - way[1]) * chunks + j for way in ways]

        @pl.when(j == 0)
        def _():
            for copy in loads:
                copy.wait()

        line_copy(ways[1], steps - ways[1][1], j).wait_recv()

        @pl.when(edge == 0)
        def _():
            line_in[upper, slot_of[0]] = jnp.zeros((rows, cols), bf16)

        @pl.when(edge > 0)
        def _():
            line_copy(ways[0], steps - edge, j).wait_recv()

        i = edge * (chunks // 2) + j // 2
        for b in range(blocks):
            exponent = exponents[0, b]
            scale = (jnp.int32(1) << exponent).astype(f32)
            inverse = (jnp.int32(1) << (15 - exponent)).astype(f32) * (2.0 ** -15)
            at = pl.ds(b * block_rows, block_rows)
            gradient = (
                mine[i, upper, j % 2, at, :].astype(f32)
                + got[i, upper, j % 2, at, :].astype(f32)
                + line_in[upper, slot_of[0], at, :].astype(f32)
                + line_in[1 - upper, slot_of[1], at, :].astype(f32)
            )
            stepped = par_v[at, lanes(j)] - factor * gradient
            levels = jnp.clip((stepped - est_v[at, lanes(j)]) * inverse, -1.0, 1.0).astype(bf16)
            own[j, at, :] = (levels.astype(f32) * scale).astype(bf16)
            out_params[0, at, lanes(j)] = stepped
        @pl.when(j >= relayed)
        def _():
            far_copy(j).start()

        for k in range(PARTS):
            near_copy(j, k).start()
        compressed = own[j].astype(f32)
        out_estimate[0, :, lanes(j)] = est_v[:, lanes(j)] + compressed
        out_mixed[0, :, lanes(j)] = mix_v[:, lanes(j)] + weight_self * compressed

    def forward(j):
        for k in range(PARTS):
            near_copy(j, k).wait_recv()

            @pl.when(j < relayed)
            def _(k=k):
                relay_copy(j, k).start()

    def finish(j):
        @pl.when(j < relayed)
        def _():
            for k in range(PARTS):
                relay_copy(j, k).wait_recv()

        @pl.when(j >= relayed)
        def _():
            far_copy(j).wait_recv()

        total = (
            out_mixed[0, :, lanes(j)] + weight_near * near[j].astype(f32) + weight_far * far[j].astype(f32)
        )
        out_mixed[0, :, lanes(j)] = total
        out_params[0, :, lanes(j)] = out_params[0, :, lanes(j)] + mixing_rate * (
            total - out_estimate[0, :, lanes(j)]
        )

    def head(s, j):
        @pl.when(edge == 0)
        def _():
            for half in (0, 1):
                if j == 1 and half == 0:
                    sent(0, 0)
                pass_on(ways[0], s, jnp.int32(2 * j + half))

    with jax.named_scope("lead"):
        grad_copy(0).wait()
        load_block(lead * 2 + other, 0).wait()
    with jax.named_scope("lead1"):
        turn(lead * 2 + other)
        put(give, 0, lead_which, product(lead, other, 0))
    with jax.named_scope("barrier"):
        pl.semaphore_wait(barrier, greeted)
        for half in (0, 1):
            first_copy(half).start()
    with jax.named_scope("lead2"):
        load_block(lead * 2 + core, 1).wait()
        turn(lead * 2 + core)
        keep_half(lead, lead_which, 0)
        for half in (0, 1):
            first_copy(half).wait_recv()

            @pl.when(edge == 0)
            def _(half=half):
                pass_on(ways[0], 0, jnp.int32(half))

    with jax.named_scope("lead3"):
        grad_copy(1).wait()
        give_half(lead, lead_which, 1)
        keep_half(lead, lead_which, 1)
        load_block(lead_next * 2 + other, 2).wait()
        turn(lead_next * 2 + other)
        give_half(lead_next, lead_which, 2)
        load_block(lead_next * 2 + core, 3).wait()
        turn(lead_next * 2 + core)
        keep_half(lead_next, lead_which, 2)
        for block in range(4, members - 4):
            load_block(block, 6).start()
        for k in range(2, len(bounds) - 1):
            grad_copy(k).start()

    def both_trails(parity, sem):
        block = act_v.at[pl.ds(0, 2)]
        pltpu.make_async_copy(block, block, act_sem.at[sem]).wait()
        turn(trail * 2 + parity)
        turn(trail_next * 2 + parity)

    with jax.named_scope("trail"):
        both_trails(other, 4)
        give_half(trail, 1 - lead_which, 0)
        half_copy(1, lead_which).wait_recv()
        head(0, 1)
        give_half(trail, 1 - lead_which, 1)
        give_half(trail_next, 1 - lead_which, 2)
    with jax.named_scope("trail2"):
        both_trails(core, 5)
        for h, dest in enumerate((trail, trail, trail_next)):
            keep_half(dest, 1 - lead_which, h)
        for copy in loads:
            copy.start()
        half_copy(2, lead_which).wait_recv()
        head(1, 0)
        for h in range(3):
            half_copy(h, 1 - lead_which).wait_recv()

    def turn_four(b):
        if members > 8:
            @pl.when(b == 2)
            def _():
                block = act_v.at[pl.ds(4, members - 8)]
                pltpu.make_async_copy(block, block, act_sem.at[6]).wait()

            for parity in (0, 1):
                for dest in (b, chips - 1 - b):
                    turn(dest * 2 + parity)

    sent_early = (4, 2)
    ready = [2, 1] + [0] * pairs

    def body(d, carry):
        for half in (0, 1):
            r = 2 * d + half
            for s in range(steps):
                odd_half = (half - begin[s]) % 2
                with jax.named_scope(f"pass{s}"):
                    if s < pairs and odd_half == 0:
                        guarded(
                            functools.partial(exchanged, s),
                            (r - begin[s]) // 2, chunks // 2, ready[s],
                        )
                    @pl.when(edge == 0)
                    def _(s=s, r=r):
                        pace(s, r)

                    for way in ways:
                        least = jnp.where(way[1] == 0, sent_early[s], 0) if s < 2 else 0
                        pass_on(way, s, r - LAG * way[1] - begin[s], least)
                if half == 0 and s == 0 and pairs > 2:
                    guarded(turn_four, d + 1, pairs, 2)
                if half == 0 and s < pairs:
                    with jax.named_scope(f"mult{s}"):
                        guarded(functools.partial(multiply, s), d + 1 - s, chunks // 2, ready[s])
            with jax.named_scope("compress"):
                guarded(compress, r - first, chunks)
            with jax.named_scope("forward"):
                guarded(forward, r - first - RELAY, chunks)
            with jax.named_scope("finish"):
                guarded(finish, r - first - GOSSIP, chunks)
        return carry

    turns = (chunks + first + 1) // 2
    lax.fori_loop(0, turns, body, 0)

    with jax.named_scope("tail"):
        for t in range(2 * turns - first, chunks + max(RELAY, GOSSIP)):
            if 0 <= t - GOSSIP < chunks:
                finish(t - GOSSIP)
            if 0 <= t - RELAY < chunks:
                forward(t - RELAY)


    with jax.named_scope("drain"):
        to_sibling((), half_r.at[0, 0]).wait_send()
        for way in ways:
            for s in range(steps):
                @pl.when(jnp.logical_and(way[1] > 0, steps - s > way[1]))
                def _(way=way, s=s):
                    whole = line_out.at[way[0], pl.ds(s * chunks, chunks)]
                    pltpu.make_async_remote_copy(
                        src_ref=whole, dst_ref=whole, send_sem=line_s.at[line_slot(way, s, 0)],
                        recv_sem=line_r.at[way[0], s, 0],
                        device_id={"mem": way[2]}, device_id_type=MESH,
                    ).wait_send()

        @pl.when(edge == 0)
        def _():
            for s in range(1 if late else 0, steps):
                sent(s, chunks - 1)
            if late:
                sent(2, chunks - 2)

        to_group(own, near, near_to, near_s, near_r.at[0, 0], ()).wait_send()
        to_group(own, far, far_to, far_s, far_r.at[0, 0], ()).wait_send()


def flush(pieces, *refs):
    sources, targets, sems = refs[:3], refs[3:6], refs[6]
    rows = sources[0].shape[1] // pieces
    copies = [
        pltpu.make_async_copy(
            sources[a].at[:, pl.ds(k * rows, rows)], targets[a].at[:, pl.ds(k * rows, rows)], sems.at[a, k]
        )
        for k in range(pieces)
        for a in range(3)
    ]
    for copy in copies:
        copy.start()
    for copy in copies:
        copy.wait()


def on_device(members, groups, params, estimate, mixed, acts, grads, exponents, edges):
    rows, width = params.shape[1:]
    tokens = acts.shape[0]
    chunks = CHUNKS
    cols = width // chunks
    chips = members // 2
    items = chips // 2 * chunks // 2
    slots = (chips - 1) * chunks
    ring = 6 if chips <= 4 else chunks
    span = RING if groups <= 4 else chunks
    factor = step_size / math.sqrt(members * tokens)
    cfg = (members, groups, chunks, rows, width, tokens, factor)
    wide = (chunks, rows, cols)
    tall = (items, 2, 2, rows, cols)
    dma = pltpu.SemaphoreType.DMA
    any_spec = pl.BlockSpec(memory_space=pl.ANY)
    smem = pl.BlockSpec(memory_space=pltpu.SMEM)
    vmem = pl.BlockSpec(memory_space=pltpu.VMEM)
    results = pl.pallas_call(
        functools.partial(kernel, cfg),
        out_shape=[pltpu.VMEM(params.shape, f32)] * 3,
        in_specs=[any_spec] * 5 + [smem] * 2,
        out_specs=[vmem] * 3,
        scratch_shapes=[
            pltpu.VMEM((members, tokens, rows), bf16),
            pltpu.VMEM((members, rows, tokens), bf16),
            pltpu.VMEM((tokens, width), bf16),
            *[pltpu.VMEM((rows, width), f32)] * 3,
            *[pltpu.VMEM(tall, bf16)] * 3,
            pltpu.VMEM((2, slots, rows, cols), bf16),
            pltpu.VMEM((2, slots + chunks, rows, cols), bf16),
            *[pltpu.VMEM(wide, bf16)] * 3,
            dma((7 if members > 8 else 6,)), dma((chunks.bit_length() - 1,)), dma((3,)),
            dma, dma((3, 2)), dma, dma((chips // 2, SLOTS)),
            dma((2 * (chips - 1) + chips // 2 - 1,)), dma((2, chips - 1, ring)),
            dma, dma((span, PARTS)), dma, dma((span + DIRECT, PARTS)),
        ],
        compiler_params=pltpu.CompilerParams(
            collective_id=0, has_side_effects=True, vmem_limit_bytes=53 * 1024 * 1024
        ),
    )(params, estimate, mixed, acts, grads, exponents, edges)
    pieces = math.gcd(PIECES, rows // 8)
    return pl.pallas_call(
        functools.partial(flush, pieces),
        out_shape=[jax.ShapeDtypeStruct(params.shape, f32)] * 3,
        in_specs=[vmem] * 3,
        out_specs=[any_spec] * 3,
        scratch_shapes=[dma((3, pieces))],
        compiler_params=pltpu.CompilerParams(vmem_limit_bytes=1024 * 1024),
    )(*results)


def solution(mesh):
    shard = P("grp", "mem", None)
    tokens = P(("grp", "mem"), None)
    return jax.shard_map(
        functools.partial(on_device, mesh.shape["mem"], mesh.shape["grp"]),
        mesh=mesh,
        in_specs=(shard, shard, shard, tokens, tokens, P("grp", "mem"), P()),
        out_specs=(shard, shard, shard),
        check_vma=False,
    )
```

```python
import functools
import math

import jax
import jax.numpy as jnp
from jax import lax
from jax.experimental import pallas as pl
from jax.experimental.pallas import tpu as pltpu
from jax.sharding import PartitionSpec as P

step_size = 0.5
mixing_rate = 0.4
CHUNKS = 16
LAG = 1
RELAY = 1
GOSSIP = 2
DIRECT = 1
PIECES = 1
SLOTS = 2
STEP = 1
RING = 5
PARTS = 2
MESH = pl.DeviceIdType.MESH
f32 = jnp.float32
bf16 = jnp.bfloat16


def kernel(
    cfg,
    params, estimate, mixed, acts, grads, exponents, edges,
    out_params, out_estimate, out_mixed,
    act_v, act_t, grad_v, par_v, est_v, mix_v,
    mine, give, got, line_out, line_in, own, near, far,
    act_sem, grad_sem, load_sem,
    pair_s, half_r, first_r, pair_r, line_s, line_r, near_s, near_r, far_s, far_r,
):
    members, groups, chunks, rows, width, tokens, factor = cfg
    chips = members // 2
    pairs = chips // 2
    steps = chips - 1
    cols = width // chunks
    g = lax.axis_index("grp")
    m = lax.axis_index("mem")
    chip, core = m // 2, m % 2
    other = 1 - core
    sibling = chip * 2 + other
    upper = jnp.where(chip < pairs, 0, 1)
    edge = jnp.where(chip < pairs, chip, chips - 1 - chip)
    inward = lax.rem(chip + chips + 1 - 2 * upper, chips) * 2 + core
    outward = lax.rem(chip + chips - 1 + 2 * upper, chips) * 2 + core
    ways = ((upper, edge, inward, 0), (1 - upper, chips - 1 - edge, outward, 1))
    odd = g % 2
    near_to = lax.rem(g + groups + 1 - 2 * odd, groups)
    far_to = lax.rem(g + groups - 1 + 2 * odd, groups)
    onward = lax.rem(g + groups + 2 - 4 * odd, groups)
    backward = lax.rem(g + groups - 2 + 4 * odd, groups)

    begin = [2 * s for s in range(pairs)]
    for s in range(pairs, steps):
        begin.append(begin[-1] + STEP)
    first = max(begin[steps - p] + LAG * p for p in range(1, chips))

    def load_block(block, sem):
        return pltpu.make_async_copy(
            acts.at[:, pl.ds(pl.multiple_of(block * rows, rows), rows)], act_v.at[block], act_sem.at[sem]
        )

    def lanes(j):
        return pl.ds(pl.multiple_of(j * cols, cols), cols)

    bounds = [0, 2]
    while bounds[-1] < chunks:
        bounds.append(min(2 * bounds[-1], chunks))

    def grad_copy(k):
        at = pl.ds(bounds[k] * cols, (bounds[k + 1] - bounds[k]) * cols)
        return pltpu.make_async_copy(grads.at[:, at], grad_v.at[:, at], grad_sem.at[k])

    loads = [
        pltpu.make_async_copy(src.at[0], dst, load_sem.at[k])
        for k, (src, dst) in enumerate(((params, par_v), (estimate, est_v), (mixed, mix_v)))
    ]

    def to_sibling(at, recv_sem):
        return pltpu.make_async_remote_copy(
            src_ref=give.at[at] if at else give, dst_ref=got.at[at] if at else got,
            send_sem=pair_s, recv_sem=recv_sem,
            device_id={"mem": sibling}, device_id_type=MESH,
        )

    half_at = (0, 1, chunks // 2)
    half_of_width = (0, 1, 0)

    def half_copy(h, which):
        return to_sibling((half_at[h], which), half_r.at[h, which])

    def first_copy(half):
        return to_sibling((0, lead_which, half), half_r.at[0, lead_which] if half == 0 else first_r)

    def pair_copy(b, j):
        return to_sibling((b * (chunks // 2) + j,), pair_r.at[b, j % SLOTS])

    ring = line_r.shape[2]

    def line_slot(way, s, j):
        if way[3]:
            return 2 * steps + jnp.minimum(s, pairs - 2)
        return 2 * s + jnp.where(way[1] == 0, j % 2, 0)

    def line_copy(way, s, j):
        return pltpu.make_async_remote_copy(
            src_ref=line_out.at[way[0], s * chunks + j], dst_ref=line_in.at[way[0], s * chunks + j],
            send_sem=line_s.at[line_slot(way, s, j)], recv_sem=line_r.at[way[0], s, j % ring],
            device_id={"mem": way[2]}, device_id_type=MESH,
        )

    def to_group(src, dst, peer, send_sem, recv_sem, at):
        return pltpu.make_async_remote_copy(
            src_ref=src.at[at] if at else src, dst_ref=dst.at[at] if at else dst,
            send_sem=send_sem, recv_sem=recv_sem,
            device_id={"grp": peer}, device_id_type=MESH,
        )

    span = near_r.shape[0]
    relayed = chunks - DIRECT

    def part_of(j, k):
        return (j, pl.ds(k * (rows // PARTS), rows // PARTS))

    def near_copy(j, k):
        return to_group(own, near, near_to, near_s, near_r.at[j % span, k], part_of(j, k))

    def relay_copy(j, k):
        return to_group(near, far, onward, far_s, far_r.at[j % span, k], part_of(j, k))

    def far_copy(j):
        return to_group(own, far, far_to, far_s, far_r.at[span + j - relayed, 0], (j,))

    def guarded(run, j, count, least=0):
        @pl.when(jnp.logical_and(j >= least, j < count))
        def _():
            run(j)

    lead_which = 1 - upper
    lead = jnp.where(chip < pairs, chips - 1, 0)
    trail = chips - 1 - lead
    lead_next = jnp.where(chip < pairs, chips - 2, 1)
    trail_next = chips - 1 - lead_next

    grad_copy(0).start()
    load_block(lead * 2 + other, 0).start()

    barrier = pltpu.get_barrier_semaphore()
    for peer in ({"mem": sibling}, {"grp": near_to}, {"grp": far_to}, {"grp": onward}, {"grp": backward}):
        pl.semaphore_signal(barrier, inc=1, device_id=peer, device_id_type=MESH)
    pl.semaphore_signal(barrier, inc=1, device_id={"mem": inward}, device_id_type=MESH)

    @pl.when(edge > 0)
    def _():
        pl.semaphore_signal(barrier, inc=1, device_id={"mem": outward}, device_id_type=MESH)

    greeted = 7 - jnp.where(edge == 0, 1, 0)
    load_block(lead * 2 + core, 1).start()
    grad_copy(1).start()
    for parity, sem in ((other, 2), (core, 3)):
        load_block(lead_next * 2 + parity, sem).start()
    for parity, sem in ((other, 4), (core, 5)):
        for dest in (trail, trail_next):
            load_block(dest * 2 + parity, sem).start()

    def turn(block):
        act_t[block] = act_v[block].T

    def product(dest, parity, j):
        return jnp.dot(
            act_t[dest * 2 + parity],
            grad_v[:, pl.ds(pl.multiple_of(2 * j * cols, 2 * cols), 2 * cols)],
            preferred_element_type=f32,
        ).astype(bf16)

    def put(ref, i, which, value):
        for half in (0, 1):
            ref[i, which, half] = value[:, half * cols : (half + 1) * cols]

    def give_half(dest, which, h):
        put(give, half_at[h], which, product(dest, other, half_of_width[h]))
        half_copy(h, which).start()

    def keep_half(dest, which, h):
        put(mine, half_at[h], which, product(dest, core, half_of_width[h]))

    def multiply(b, j):
        i = b * (chunks // 2) + j
        if b == 0:
            for k in range(len(bounds) - 1):
                @pl.when(2 * j == bounds[k])
                def _(k=k):
                    grad_copy(k).wait()
        for which, dest in ((0, b), (1, chips - 1 - b)):
            put(give, i, which, product(dest, other, j))
        pair_copy(b, j).start()
        for which, dest in ((0, b), (1, chips - 1 - b)):
            put(mine, i, which, product(dest, core, j))

    def exchanged(b, j):
        pair_copy(b, j).wait_recv()

    def pair_sum(i, which, half):
        return mine[i, which, half].astype(f32) + got[i, which, half].astype(f32)

    def pass_on(way, s, j, least=0):
        far_dest = steps - s
        b = min(s, steps - s)
        which = 1 - way[0] if far_dest >= pairs else way[0]
        i = b * (chunks // 2) + j // 2
        slot = s * chunks + j

        @pl.when(jnp.logical_and(far_dest > way[1], jnp.logical_and(j >= least, j < chunks)))
        def _():
            @pl.when(way[1] == 0)
            def _():
                line_out[way[0], slot] = pair_sum(i, which, j % 2).astype(bf16)

            @pl.when(way[1] > 0)
            def _():
                line_copy(way, s, j).wait_recv()
                line_out[way[0], slot] = (
                    pair_sum(i, which, j % 2) + line_in[way[0], slot].astype(f32)
                ).astype(bf16)

            line_copy(way, s, j).start()

    def sent(s, j):
        line_copy(ways[0], s, j).wait_send()

    late = begin == [0, 2, 3]

    def pace(s, r):
        j = r - begin[s]

        @pl.when(jnp.logical_and(r > (4 if s == 0 else 3), jnp.logical_and(j >= 1, (r if late else j) < chunks)))
        def _():
            sent(s, j - 1)

        turns = {0: ((4, 1, 0),), 1: ((2, 0, 1), (3, 0, 2)), 2: ((3, 0, 3),)}.get(s, ())
        if late:
            turns += {
                1: ((chunks, 0, chunks - 1), (chunks + 1, 2, chunks - 4)),
                2: ((chunks, 1, chunks - 3), (chunks + 1, 1, chunks - 2), (chunks + 2, 2, chunks - 3)),
            }.get(s, ())
        for at, step, chunk in turns:
            @pl.when(r == at)
            def _(step=step, chunk=chunk):
                sent(step, chunk)

    weight_right = edges[g]
    weight_left = edges[lax.rem(g + groups - 1, groups)]
    weight_self = 1.0 - weight_left - weight_right
    weight_near = jnp.where(odd == 1, weight_left, weight_right)
    weight_far = jnp.where(odd == 1, weight_right, weight_left)
    blocks = exponents.shape[1]
    block_rows = rows // blocks

    def compress(j):
        slot_of = [(steps - way[1]) * chunks + j for way in ways]

        @pl.when(j == 0)
        def _():
            for copy in loads:
                copy.wait()

        line_copy(ways[1], steps - ways[1][1], j).wait_recv()

        @pl.when(edge == 0)
        def _():
            line_in[upper, slot_of[0]] = jnp.zeros((rows, cols), bf16)

        @pl.when(edge > 0)
        def _():
            line_copy(ways[0], steps - edge, j).wait_recv()

        i = edge * (chunks // 2) + j // 2
        for b in range(blocks):
            exponent = exponents[0, b]
            scale = (jnp.int32(1) << exponent).astype(f32)
            inverse = (jnp.int32(1) << (15 - exponent)).astype(f32) * (2.0 ** -15)
            at = pl.ds(b * block_rows, block_rows)
            gradient = (
                mine[i, upper, j % 2, at, :].astype(f32)
                + got[i, upper, j % 2, at, :].astype(f32)
                + line_in[upper, slot_of[0], at, :].astype(f32)
                + line_in[1 - upper, slot_of[1], at, :].astype(f32)
            )
            stepped = par_v[at, lanes(j)] - factor * gradient
            levels = jnp.clip((stepped - est_v[at, lanes(j)]) * inverse, -1.0, 1.0).astype(bf16)
            own[j, at, :] = (levels.astype(f32) * scale).astype(bf16)
            out_params[0, at, lanes(j)] = stepped
        @pl.when(j >= relayed)
        def _():
            far_copy(j).start()

        for k in range(PARTS):
            near_copy(j, k).start()
        compressed = own[j].astype(f32)
        out_estimate[0, :, lanes(j)] = est_v[:, lanes(j)] + compressed
        out_mixed[0, :, lanes(j)] = mix_v[:, lanes(j)] + weight_self * compressed

    def forward(j):
        for k in range(PARTS):
            near_copy(j, k).wait_recv()

            @pl.when(j < relayed)
            def _(k=k):
                relay_copy(j, k).start()

    def finish(j):
        @pl.when(j < relayed)
        def _():
            for k in range(PARTS):
                relay_copy(j, k).wait_recv()

        @pl.when(j >= relayed)
        def _():
            far_copy(j).wait_recv()

        total = (
            out_mixed[0, :, lanes(j)] + weight_near * near[j].astype(f32) + weight_far * far[j].astype(f32)
        )
        out_mixed[0, :, lanes(j)] = total
        out_params[0, :, lanes(j)] = out_params[0, :, lanes(j)] + mixing_rate * (
            total - out_estimate[0, :, lanes(j)]
        )

    def head(s, j):
        @pl.when(edge == 0)
        def _():
            for half in (0, 1):
                if j == 1 and half == 0:
                    sent(0, 0)
                pass_on(ways[0], s, jnp.int32(2 * j + half))

    with jax.named_scope("lead"):
        grad_copy(0).wait()
        load_block(lead * 2 + other, 0).wait()
    with jax.named_scope("lead1"):
        turn(lead * 2 + other)
        put(give, 0, lead_which, product(lead, other, 0))
    with jax.named_scope("barrier"):
        pl.semaphore_wait(barrier, greeted)
        for half in (0, 1):
            first_copy(half).start()
    with jax.named_scope("lead2"):
        load_block(lead * 2 + core, 1).wait()
        turn(lead * 2 + core)
        keep_half(lead, lead_which, 0)
        for half in (0, 1):
            first_copy(half).wait_recv()

            @pl.when(edge == 0)
            def _(half=half):
                pass_on(ways[0], 0, jnp.int32(half))

    with jax.named_scope("lead3"):
        grad_copy(1).wait()
        give_half(lead, lead_which, 1)
        keep_half(lead, lead_which, 1)
        load_block(lead_next * 2 + other, 2).wait()
        turn(lead_next * 2 + other)
        give_half(lead_next, lead_which, 2)
        load_block(lead_next * 2 + core, 3).wait()
        turn(lead_next * 2 + core)
        keep_half(lead_next, lead_which, 2)
        for block in range(4, members - 4):
            load_block(block, 6).start()
        for k in range(2, len(bounds) - 1):
            grad_copy(k).start()

    def both_trails(parity, sem):
        block = act_v.at[pl.ds(0, 2)]
        pltpu.make_async_copy(block, block, act_sem.at[sem]).wait()
        turn(trail * 2 + parity)
        turn(trail_next * 2 + parity)

    with jax.named_scope("trail"):
        both_trails(other, 4)
        give_half(trail, 1 - lead_which, 0)
        half_copy(1, lead_which).wait_recv()
        head(0, 1)
        give_half(trail, 1 - lead_which, 1)
        give_half(trail_next, 1 - lead_which, 2)
    with jax.named_scope("trail2"):
        both_trails(core, 5)
        for h, dest in enumerate((trail, trail, trail_next)):
            keep_half(dest, 1 - lead_which, h)
        for copy in loads:
            copy.start()
        half_copy(2, lead_which).wait_recv()
        head(1, 0)
        for h in range(3):
            half_copy(h, 1 - lead_which).wait_recv()

    def turn_four(b):
        if members > 8:
            @pl.when(b == 2)
            def _():
                block = act_v.at[pl.ds(4, members - 8)]
                pltpu.make_async_copy(block, block, act_sem.at[6]).wait()

            for parity in (0, 1):
                for dest in (b, chips - 1 - b):
                    turn(dest * 2 + parity)

    sent_early = (4, 2)
    ready = [2, 1] + [0] * pairs

    def body(d, carry):
        for half in (0, 1):
            r = 2 * d + half
            for s in range(steps):
                odd_half = (half - begin[s]) % 2
                with jax.named_scope(f"pass{s}"):
                    if s < pairs and odd_half == 0:
                        guarded(
                            functools.partial(exchanged, s),
                            (r - begin[s]) // 2, chunks // 2, ready[s],
                        )
                    @pl.when(edge == 0)
                    def _(s=s, r=r):
                        pace(s, r)

                    for way in ways:
                        least = jnp.where(way[1] == 0, sent_early[s], 0) if s < 2 else 0
                        pass_on(way, s, r - LAG * way[1] - begin[s], least)
                if half == 0 and s == 0 and pairs > 2:
                    guarded(turn_four, d + 1, pairs, 2)
                if half == 0 and s < pairs:
                    with jax.named_scope(f"mult{s}"):
                        guarded(functools.partial(multiply, s), d + 1 - s, chunks // 2, ready[s])
            with jax.named_scope("compress"):
                guarded(compress, r - first, chunks)
            with jax.named_scope("forward"):
                guarded(forward, r - first - RELAY, chunks)
            with jax.named_scope("finish"):
                guarded(finish, r - first - GOSSIP, chunks)
        return carry

    turns = (chunks + first + 1) // 2
    lax.fori_loop(0, turns, body, 0)

    with jax.named_scope("tail"):
        for t in range(2 * turns - first, chunks + max(RELAY, GOSSIP)):
            if 0 <= t - GOSSIP < chunks:
                finish(t - GOSSIP)
            if 0 <= t - RELAY < chunks:
                forward(t - RELAY)


    with jax.named_scope("drain"):
        to_sibling((), half_r.at[0, 0]).wait_send()
        for way in ways:
            for s in range(steps):
                @pl.when(jnp.logical_and(way[1] > 0, steps - s > way[1]))
                def _(way=way, s=s):
                    whole = line_out.at[way[0], pl.ds(s * chunks, chunks)]
                    pltpu.make_async_remote_copy(
                        src_ref=whole, dst_ref=whole, send_sem=line_s.at[line_slot(way, s, 0)],
                        recv_sem=line_r.at[way[0], s, 0],
                        device_id={"mem": way[2]}, device_id_type=MESH,
                    ).wait_send()

        @pl.when(edge == 0)
        def _():
            for s in range(1 if late else 0, steps):
                sent(s, chunks - 1)
            if late:
                sent(2, chunks - 2)

        to_group(own, near, near_to, near_s, near_r.at[0, 0], ()).wait_send()
        to_group(own, far, far_to, far_s, far_r.at[0, 0], ()).wait_send()


def flush(pieces, *refs):
    sources, targets, sems = refs[:3], refs[3:6], refs[6]
    rows = sources[0].shape[1] // pieces
    copies = [
        pltpu.make_async_copy(
            sources[a].at[:, pl.ds(k * rows, rows)], targets[a].at[:, pl.ds(k * rows, rows)], sems.at[a, k]
        )
        for k in range(pieces)
        for a in range(3)
    ]
    for copy in copies:
        copy.start()
    for copy in copies:
        copy.wait()


def on_device(members, groups, params, estimate, mixed, acts, grads, exponents, edges):
    rows, width = params.shape[1:]
    tokens = acts.shape[0]
    chunks = CHUNKS
    cols = width // chunks
    chips = members // 2
    items = chips // 2 * chunks // 2
    slots = (chips - 1) * chunks
    ring = 6 if chips <= 4 else chunks
    span = RING if groups <= 4 else chunks
    factor = step_size / math.sqrt(members * tokens)
    cfg = (members, groups, chunks, rows, width, tokens, factor)
    wide = (chunks, rows, cols)
    tall = (items, 2, 2, rows, cols)
    dma = pltpu.SemaphoreType.DMA
    any_spec = pl.BlockSpec(memory_space=pl.ANY)
    smem = pl.BlockSpec(memory_space=pltpu.SMEM)
    vmem = pl.BlockSpec(memory_space=pltpu.VMEM)
    results = pl.pallas_call(
        functools.partial(kernel, cfg),
        out_shape=[pltpu.VMEM(params.shape, f32)] * 3,
        in_specs=[any_spec] * 5 + [smem] * 2,
        out_specs=[vmem] * 3,
        scratch_shapes=[
            pltpu.VMEM((members, tokens, rows), bf16),
            pltpu.VMEM((members, rows, tokens), bf16),
            pltpu.VMEM((tokens, width), bf16),
            *[pltpu.VMEM((rows, width), f32)] * 3,
            *[pltpu.VMEM(tall, bf16)] * 3,
            pltpu.VMEM((2, slots, rows, cols), bf16),
            pltpu.VMEM((2, slots + chunks, rows, cols), bf16),
            *[pltpu.VMEM(wide, bf16)] * 3,
            dma((7 if members > 8 else 6,)), dma((chunks.bit_length() - 1,)), dma((3,)),
            dma, dma((3, 2)), dma, dma((chips // 2, SLOTS)),
            dma((2 * (chips - 1) + chips // 2 - 1,)), dma((2, chips - 1, ring)),
            dma, dma((span, PARTS)), dma, dma((span + DIRECT, PARTS)),
        ],
        compiler_params=pltpu.CompilerParams(
            collective_id=0, has_side_effects=True, vmem_limit_bytes=53 * 1024 * 1024
        ),
    )(params, estimate, mixed, acts, grads, exponents, edges)
    pieces = math.gcd(PIECES, rows // 8)
    return pl.pallas_call(
        functools.partial(flush, pieces),
        out_shape=[jax.ShapeDtypeStruct(params.shape, f32)] * 3,
        in_specs=[vmem] * 3,
        out_specs=[any_spec] * 3,
        scratch_shapes=[dma((3, pieces))],
        compiler_params=pltpu.CompilerParams(vmem_limit_bytes=1024 * 1024),
    )(*results)


def solution(mesh):
    shard = P("grp", "mem", None)
    tokens = P(("grp", "mem"), None)
    return jax.shard_map(
        functools.partial(on_device, mesh.shape["mem"], mesh.shape["grp"]),
        mesh=mesh,
        in_specs=(shard, shard, shard, tokens, tokens, P("grp", "mem"), P()),
        out_specs=(shard, shard, shard),
        check_vma=False,
    )
```
